256 devices in a mesh: gy: 32 (over z, x), gx: 8 (over y, core).
Axes of the slice: x: 4, y: 4, z: 8, core: 2. Of those that a mesh axis runs over, the one named last changes fastest.
Arguments:
- right_side: float32 [32, 2048, 1024], P(None, 'gy', 'gx'), may hold values from -32 to 32
- couplings: float32 [3, 2048, 1024], P(None, 'gy', 'gx'), may hold values from 0.1 to 0.5
- center: float32 [2048, 1024], P('gy', 'gx'), may hold values from 0.6 to 1.5
- ocean_mask: int32 [2048, 1024], P('gy', 'gx'), may hold values 0 or 1
Outputs:
- solution: float32 [32, 2048, 1024], P(None, 'gy', 'gx')
- residual: float32 [32, 2048, 1024], P(None, 'gy', 'gx')
The draws below stay inside these ranges and needn't reach their ends.
All inputs are finite; a program needn't handle non-finite values. No bound on the sum of `ocean_mask` on one device may be relied on, other than what follows from the above.
Results may differ from the reference program's by a relative error of at most 0.0055.
Values sent between devices are 32-bit elements; how exact they have to be, the bound alone decides.
No kernel may reach another device: no remote copies, remote signals or barrier semaphores. Data moves between devices by JAX's collectives and lax.ppermute only.
A program may use at most 64 MiB of HBM per device.

```python
import math
import jax
import jax.numpy as jnp
from jax import lax

MEMBERS = 32
ITERS = 6
NLAT = 2048
NLON = 1024


def draw_right_side(key, part):
    key_base = jax.random.fold_in(key, 0)
    latitude = jnp.arange(NLAT, dtype=jnp.float32) / max(NLAT - 1, 1)
    rising = (1.0 + 2.0 * latitude)[None, :, None]
    base = jnp.clip(jax.random.normal(key_base, (MEMBERS, NLAT, NLON), jnp.float32), -5.0, 5.0)
    return base * rising


def place_ends(array, stream_key, least, top_value):
    longest = array.shape.index(max(array.shape))
    spots = []
    for shift in (0, 1):
        where = [jax.random.randint(jax.random.fold_in(stream_key, axis), (), 0, length) for axis, length in enumerate(array.shape)]
        where[longest] = (where[longest] + shift) % array.shape[longest]
        spots.append(tuple(where))
    return array.at[spots[0]].set(least).at[spots[1]].set(top_value)


def block_levels(key, extent, cuts, least, top_value):
    level = 1.0
    for dim, parts in cuts:
        steps = jax.random.uniform(jax.random.fold_in(jax.random.fold_in(key, 6), dim), (parts,), jnp.float32, least / len(cuts), top_value / len(cuts))
        level = level * jnp.repeat(jnp.exp(steps), extent[dim] // parts).reshape((-1,) + (1,) * (len(extent) - 1 - dim))
    return level


def setup_inputs(seed: int = 0) -> dict:
    keys = jax.random.split(jax.random.key(seed), 5)
    return {
        "right_side": draw_right_side(jax.random.fold_in(keys[4], 71), 0),
        "couplings": jnp.clip(jnp.exp(math.log(0.5) - 1.609438 * jax.random.uniform(keys[1], (3, NLAT, NLON), jnp.float32) ** block_levels(keys[1], (3, NLAT, NLON), ((1, 32), (2, 8)), -0.2, 0.2)), 0.1, 0.5),
        "center": jnp.clip(jnp.exp(math.log(1.5) - 0.9162907 * jax.random.uniform(keys[2], (NLAT, NLON), jnp.float32) ** block_levels(keys[2], (NLAT, NLON), ((0, 32), (1, 8)), -0.2, 0.2)), 0.6, 1.5),
        "ocean_mask": place_ends((jax.random.randint(keys[3], (NLAT, NLON), 0, 10) < 9).astype(jnp.int32), jax.random.fold_in(keys[3], 1), 0, 1),
    }


def extend_field(field):
    north_row = field[-1, ::-1]
    lat_padded = jnp.concatenate([jnp.zeros((1, field.shape[1]), jnp.float32), field, north_row[None, :]], axis=0)
    return jnp.concatenate([lat_padded[:, -1:], lat_padded, lat_padded[:, :1]], axis=1)


def coupling_terms(couplings):
    north_c = couplings[0]
    east_c = couplings[1]
    corner_c = couplings[2]
    zero_row = jnp.zeros((1, north_c.shape[1]), jnp.float32)
    north_s = jnp.concatenate([zero_row, north_c[:-1]], axis=0)
    east_w = jnp.roll(east_c, 1, axis=1)
    corner_s = jnp.concatenate([zero_row, corner_c[:-1]], axis=0)
    corner_w = jnp.roll(corner_c, 1, axis=1)
    corner_sw = jnp.roll(corner_s, 1, axis=1)
    return (north_c, north_s, east_c, east_w, corner_c, corner_s, corner_w, corner_sw)


def operate(field, terms, diag_total, oceanf):
    padded = extend_field(field)
    beside = terms[0] * padded[2:, 1:-1] + terms[1] * padded[:-2, 1:-1]
    beside = beside + terms[2] * padded[1:-1, 2:] + terms[3] * padded[1:-1, :-2]
    beside = beside + terms[4] * padded[2:, 2:] + terms[5] * padded[:-2, 2:]
    beside = beside + terms[6] * padded[2:, :-2] + terms[7] * padded[:-2, :-2]
    return oceanf * (diag_total * field - beside)


def reference(right_side, couplings, center, ocean_mask):
    oceanf = ocean_mask.astype(jnp.float32)
    terms = coupling_terms(couplings)
    diag_total = center + terms[0] + terms[1] + terms[2] + terms[3] + terms[4] + terms[5] + terms[6] + terms[7]
    inverse = oceanf / diag_total

    def solve_one(member_rhs):
        residual = member_rhs * oceanf
        precond = residual * inverse
        direction = precond
        rz_now = jnp.sum(residual * precond)
        solution = jnp.zeros_like(residual)
        for iteration in range(ITERS):
            image_field = operate(direction, terms, diag_total, oceanf)
            step_size = rz_now / jnp.sum(direction * image_field)
            solution = solution + step_size * direction
            residual = residual - step_size * image_field
            precond = residual * inverse
            rz_new = jnp.sum(residual * precond)
            direction = precond + (rz_new / rz_now) * direction
            rz_now = rz_new
        return solution, residual

    solution, residual = lax.map(solve_one, right_side)
    return (solution, residual)
```

```python
import jax
import jax.numpy as jnp
from jax import lax
from jax.experimental import pallas as pl
from jax.experimental.pallas import tpu as pltpu
from jax.sharding import Mesh
from jax.sharding import PartitionSpec as P

ITERS = 6
SHIFT = (0.375, 0.0, 0.375, 0.0, 0.375, 0.0)
GY = ("gy_0", "gy_1")
GX = ("gx_0", "gx_1")
ALL = GY + GX
MEMBERS = 32
ROWS = 64
LANES = 128
HALO = 8
TILES = (ROWS + 2 * HALO) // 8
EXT = ROWS + 2 * HALO
GROUPS = MEMBERS // 4
PLANES = 4
BASIS = ITERS + 1
PAIRS = [(i, j) for i in range(ITERS) for j in range(i, BASIS)]
INTERPRET = False
F32 = jnp.float32
VMEM = pl.BlockSpec(memory_space=pltpu.VMEM)
SMEM = pl.BlockSpec(memory_space=pltpu.SMEM)


def lanes_of():
    return lax.broadcasted_iota(jnp.int32, (8, LANES), 1)


def slot_of(member):
    return 32 * (member % 4) + 8 * (member // 4 % 4)


def pack_kernel(right_ref, planes_ref, south_ref, north_ref, fold_ref, west_ref, east_ref, ghost_ref):
    window = lanes_of() // 8

    def one(load, tile):
        for h in range(3):
            members = range(16 * h, 16 * h + 16) if h < 2 else range(MEMBERS, MEMBERS + PLANES)
            first = last = None
            for m in members:
                value = load(m)
                slot = slot_of(m) if h < 2 else 32 * (m - MEMBERS)
                low = value if slot == 0 else pltpu.roll(value, slot, 1)
                high = pltpu.roll(value, (slot + 8) % LANES, 1)
                if first is None:
                    first, last = low, high
                else:
                    first = jnp.where(window == slot // 8, low, first)
                    last = jnp.where(window == slot // 8, high, last)
            west_ref[h, tile] = first
            east_ref[h, tile] = last

    def own(t, _):
        at = pl.multiple_of(8 * t, 8)

        def load(m):
            if m < MEMBERS:
                return right_ref[m, pl.ds(at, 8), :]
            return planes_ref[m - MEMBERS, pl.ds(at, 8), :]

        one(load, t + 1)
        return 0

    lax.fori_loop(0, ROWS // 8, own, 0)
    one(lambda m: south_ref[m], 0)

    def north(m):
        value = north_ref[m] + fold_ref[m]
        ghost_ref[m] = value
        return value

    one(north, TILES - 1)


def basis_kernel(
    top_ref, right_ref, planes_ref, south_ref, north_ref, own_west_ref, own_east_ref, from_west_ref, from_east_ref,
    basis_ref, diag_ref, gram_ref,
    strip_ref, plane_ref, plane_strip_ref, weight_ref, weight_strip_ref, inverse_ref, inverse_strip_ref, partial_ref,
):
    lane = lanes_of()
    spot = lane % 32

    def main_row(member, tile):
        return 8 + member * EXT + 8 * tile

    zero = jnp.zeros((8, LANES), F32)
    for j in range(ITERS):
        basis_ref[j, 0:8] = zero
        basis_ref[j, 8 + MEMBERS * EXT : 16 + MEMBERS * EXT] = zero
        strip_ref[j, 0:8] = zero
        strip_ref[j, 8 + GROUPS * EXT : 16 + GROUPS * EXT] = zero

    for p in range(PLANES):
        base = 8 + p * EXT
        plane_ref[base : base + 8] = south_ref[MEMBERS + p]
        plane_ref[base + 8 : base + 8 + ROWS] = planes_ref[p]
        plane_ref[base + 8 + ROWS : base + EXT] = north_ref[MEMBERS + p]
    plane_ref[0:8] = zero
    plane_ref[8 + PLANES * EXT : 16 + PLANES * EXT] = zero
    plane_strip_ref[0:8] = zero
    plane_strip_ref[8 + PLANES * EXT : 16 + PLANES * EXT] = zero

    def joined(h, tile, at):
        def moved(value, shift):
            shift %= LANES
            return value if shift == 0 else pltpu.roll(value, shift, 1)

        out = moved(from_west_ref[h, tile], -at)
        out = jnp.where(spot < 8, out, moved(own_west_ref[h, tile], 8 - at))
        out = jnp.where(spot < 16, out, moved(own_east_ref[h, tile], 16 - at))
        return jnp.where(spot < 24, out, moved(from_east_ref[h, tile], 24 - at))

    def plane_strips(t, _):
        value = joined(2, t, 0)
        for p in range(PLANES):
            one = jnp.where(lane // 32 == p, value, 0.0)
            one = one + pltpu.roll(one, 32, 1)
            one = one + pltpu.roll(one, 64, 1)
            plane_strip_ref[pl.ds(pl.multiple_of(8 + p * EXT + 8 * t, 8), 8), :] = one
        return 0

    lax.fori_loop(0, TILES, plane_strips, 0)

    def weights(t, ghost):
        dr = 1 if ghost else -1

        def row(ref, p, shift):
            return ref[pl.ds(8 + p * EXT + 8 * t + shift, 8), :]

        def beside(main, strip):
            if ghost:
                return jnp.where(lane == 127, pltpu.roll(strip, 127 - 24, 1), pltpu.roll(main, 127, 1))
            return jnp.where(lane == 0, pltpu.roll(strip, LANES - 7, 1), pltpu.roll(main, 1, 1))

        def finish(cn0, cnr, ce0, cec, cc0, ccr, ccc, ccrc, center, weight, inverse, main):
            total = center + cn0 + cnr + ce0 + cec + cc0 + ccr + ccc + ccrc
            inv = jnp.where(center > 0.0, 1.0 / total, 0.0)
            inverse[t] = inv
            if ghost:
                w = dict(s=cn0, n=cnr, w=ce0, e=cec, sw=cc0, nw=ccr, se=ccc, ne=ccrc)
            else:
                w = dict(n=cn0, s=cnr, e=ce0, w=cec, ne=cc0, se=ccr, nw=ccc, sw=ccrc)

            def ahead(value):
                value = pltpu.roll(value * inv, 1, 1)
                return jnp.where(lane == 0, 0.0, value) if main else value

            def behind(value):
                value = pltpu.roll(value * inv, LANES - 1, 1)
                return jnp.where(lane == LANES - 1, 0.0, value) if main else value

            for k, value in enumerate((
                w["s"] * inv, w["n"] * inv,
                ahead(w["se"]), ahead(w["e"]), ahead(w["ne"]),
                behind(w["sw"]), behind(w["w"]), behind(w["nw"]),
            )):
                weight[t, k] = value
            return total

        strips = [row(plane_strip_ref, p, 0) for p in range(PLANES)]
        strips_r = [row(plane_strip_ref, p, dr) for p in (0, 2)]
        side = LANES - 1 if ghost else 1
        finish(
            strips[0], strips_r[0], strips[1], pltpu.roll(strips[1], side, 1),
            strips[2], strips_r[1], pltpu.roll(strips[2], side, 1), pltpu.roll(strips_r[1], side, 1),
            strips[3], weight_strip_ref, inverse_strip_ref, False,
        )
        mains = [row(plane_ref, p, 0) for p in range(PLANES)]
        mains_r = [row(plane_ref, p, dr) for p in (0, 2)]
        return finish(
            mains[0], mains_r[0], mains[1], beside(mains[1], strips[1]),
            mains[2], mains_r[1], beside(mains[2], strips[2]), beside(mains_r[1], strips_r[1]),
            mains[3], weight_ref, inverse_ref, True,
        )

    weights(0, False)

    def inner_weights(t, _):
        diag_ref[pl.ds(pl.multiple_of(8 * (t - 1), 8), 8), :] = weights(t, False)
        return 0

    lax.fori_loop(1, TILES - 1, inner_weights, 0)

    @pl.when(top_ref[0] == 0)
    def _():
        weights(TILES - 1, False)

    @pl.when(top_ref[0] != 0)
    def _():
        weights(TILES - 1, True)

    def first(t, load):
        inv = inverse_ref[t]
        for m in range(MEMBERS):
            basis_ref[0, pl.ds(pl.multiple_of(main_row(m, t), 8), 8), :] = load(m) * inv
        inv = inverse_strip_ref[t]
        for s in range(GROUPS):
            strip_ref[0, pl.ds(pl.multiple_of(8 + s * EXT + 8 * t, 8), 8), :] = joined(s // 4, t, 8 * (s % 4)) * inv

    first(0, lambda m: south_ref[m])

    def inner_first(t, _):
        first(t, lambda m: right_ref[m, pl.ds(pl.multiple_of(8 * (t - 1), 8), 8), :])
        return 0

    lax.fori_loop(1, TILES - 1, inner_first, 0)
    first(TILES - 1, lambda m: north_ref[m])

    def step(j, t, strips):
        w = [weight_ref[t, k] for k in range(8)]
        ws = [weight_strip_ref[t, k] for k in range(8)]

        def parts(ref, base, w):
            a = ref[j, pl.ds(base - 1, 8), :]
            b = ref[j, pl.ds(pl.multiple_of(base, 8), 8), :]
            c = ref[j, pl.ds(base + 1, 8), :]
            middle = w[0] * a + w[1] * c
            if SHIFT[j]:
                middle = middle - SHIFT[j] * b
            return middle, (w[2] * a + w[4] * c) + w[3] * b, (w[5] * a + w[7] * c) + w[6] * b

        for s in range(GROUPS):
            base = 8 + s * EXT + 8 * t
            middle, ahead, behind = parts(strip_ref, base, ws)
            if strips:
                strip_ref[j + 1, pl.ds(pl.multiple_of(base, 8), 8), :] = (
                    middle + pltpu.roll(ahead, LANES - 1, 1) + pltpu.roll(behind, 1, 1)
                )
            edge = jnp.where(spot == 6, pltpu.roll(ahead, LANES - 18, 1), behind)
            for q in range(4):
                m = 4 * s + q
                base = main_row(m, t)
                middle, ahead, behind = parts(basis_ref, base, w)
                across = pltpu.roll(edge, (LANES - 7 - 32 * q) % LANES, 1)
                middle = middle + jnp.where((lane == 0) | (lane == LANES - 1), across, 0.0)
                basis_ref[j + 1, pl.ds(pl.multiple_of(base, 8), 8), :] = (
                    middle + pltpu.roll(ahead, LANES - 1, 1) + pltpu.roll(behind, 1, 1)
                )

    for j in range(ITERS - 1):
        def body(t, _, j=j):
            step(j, t, True)
            return 0

        lax.fori_loop(0, TILES, body, 0)

    def last_body(t, _):
        step(ITERS - 1, t, False)
        return 0

    lax.fori_loop(1, TILES - 1, last_body, 0)

    def products(m, _):
        sums = [None] * len(PAIRS)
        for t in range(1, TILES - 1):
            u = [basis_ref[j, pl.ds(pl.multiple_of(main_row(m, t), 8), 8), :] for j in range(BASIS)]
            d = diag_ref[8 * (t - 1) : 8 * t]
            scaled = [d * u[j] for j in range(ITERS)]
            for n, (i, j) in enumerate(PAIRS):
                term = scaled[i] * u[j]
                sums[n] = term if sums[n] is None else sums[n] + term
        for n in range(len(PAIRS)):
            partial_ref[pl.ds(pl.multiple_of((n * MEMBERS + m) * 8, 8), 8), :] = sums[n]
        return 0

    lax.fori_loop(0, MEMBERS, products, 0)
    result = zero
    for l in range(len(PAIRS) * MEMBERS // 8):
        rows = [partial_ref[pl.ds(64 * l + k, 8, stride=8), :] for k in range(8)]
        while len(rows) > 1:
            rows = [rows[k] + rows[k + 1] for k in range(0, len(rows), 2)]
        result = jnp.where(lane == l, jnp.sum(rows[0], axis=1, keepdims=True), result)
    gram_ref[...] = result


def two_sum(a, b):
    s = a + b
    t = s - a
    return s, (a - (s - t)) + (b - t)


def quick(a, b):
    s = a + b
    return s, b - (s - a)


def halves(a):
    t = 4097.0 * a
    high = t - (t - a)
    return high, a - high


def add2(a, b):
    s, e = two_sum(a[0], b[0])
    return quick(s, e + (a[1] + b[1]))


def mul2(a, b):
    p = a[0] * b[0]
    ah, al = halves(a[0])
    bh, bl = halves(b[0])
    e = ((ah * bh - p) + ah * bl + al * bh) + al * bl
    return quick(p, e + (a[0] * b[1] + a[1] * b[0]))


def neg2(a):
    return -a[0], -a[1]


def div2(a, b):
    q = a[0] / b[0]
    zero = jnp.zeros_like(q)
    rest = add2(a, neg2(mul2((q, zero), b)))
    return quick(q, rest[0] / b[0])


def sum2(terms):
    terms = list(terms)
    while len(terms) > 1:
        terms = [add2(terms[k], terms[k + 1]) if k + 1 < len(terms) else terms[k] for k in range(0, len(terms), 2)]
    return terms[0]


def finish_kernel(total_ref, basis_ref, diag_ref, solution_ref, residual_ref, coeff_ref):
    count = total_ref.shape[0]
    high, low = sum2([(total_ref[n, 0], total_ref[n, 1]) for n in range(count)])
    gram = {}
    for n, (i, j) in enumerate(PAIRS):
        shift = (LANES - 4 * n) % LANES
        value = (high, low) if shift == 0 else (pltpu.roll(high, shift, 1), pltpu.roll(low, shift, 1))
        gram[i, j] = gram[j, i] = value

    def scaled(value, factor):
        if factor == 1.0:
            return value
        s, e = two_sum(0.5 * value[0], 0.125 * value[0])
        return quick(s, e + factor * value[1])

    def product(a, b):
        terms = []
        for i, ai in enumerate(a):
            terms.append(mul2(ai, sum2([mul2(gram[i, j], bj) for j, bj in enumerate(b)])))
        return sum2(terms)

    one = (jnp.ones((8, LANES), F32), jnp.zeros((8, LANES), F32))
    precond, direction, answer = [one], [one], []
    rz = gram[0, 0]
    for k in range(ITERS):
        image = [scaled(c, 1.0 - SHIFT[j]) for j, c in enumerate(direction)]
        image = [image[0]] + [
            add2(image[j], neg2(direction[j - 1])) for j in range(1, k + 1)
        ] + [neg2(direction[k])]
        step_size = div2(rz, product(direction, image))
        moved = [mul2(step_size, c) for c in direction]
        answer = [add2(a, b) for a, b in zip(answer, moved)] + moved[len(answer):]
        moved = [neg2(mul2(step_size, c)) for c in image]
        precond = [add2(a, b) for a, b in zip(precond, moved)] + moved[len(precond):]
        if k + 1 < ITERS:
            rz_new = product(precond, precond)
            ratio = div2(rz_new, rz)
            moved = [mul2(ratio, c) for c in direction]
            direction = [add2(a, b) for a, b in zip(precond, moved)] + precond[len(moved):]
            rz = rz_new

    values = [c[0] for c in answer] + [c[0] for c in precond]
    for n, value in enumerate(values):
        for l in range(MEMBERS // 8):
            coeff_ref[n, 8 * l : 8 * l + 8] = jnp.broadcast_to(value[:, l : l + 1], (8, LANES))

    def combine(m, _):
        c = [jnp.broadcast_to(coeff_ref[n, pl.ds(m, 1), :], (8, LANES)) for n in range(2 * ITERS + 1)]
        for t in range(ROWS // 8):
            at = pl.multiple_of(16 + m * EXT + 8 * t, 8)
            u = [basis_ref[j, pl.ds(at, 8), :] for j in range(BASIS)]
            solved = c[0] * u[0]
            left = c[ITERS] * u[0]
            for j in range(1, BASIS):
                if j < ITERS:
                    solved = solved + c[j] * u[j]
                left = left + c[ITERS + j] * u[j]
            solution_ref[m, 8 * t : 8 * t + 8] = solved
            residual_ref[m, 8 * t : 8 * t + 8] = diag_ref[8 * t : 8 * t + 8] * left
        return 0

    lax.fori_loop(0, MEMBERS, combine, 0)


def shape(*dims):
    return jax.ShapeDtypeStruct(dims, F32)


def call(kernel, inputs, out_shape, scratch=(), name=None, in_specs=None):
    return pl.pallas_call(
        kernel,
        out_shape=out_shape,
        in_specs=in_specs or [VMEM] * len(inputs),
        out_specs=[VMEM] * len(out_shape),
        scratch_shapes=list(scratch),
        interpret=INTERPRET,
        name=name,
        compiler_params=pltpu.CompilerParams(vmem_limit_bytes=60 * 1024 * 1024),
    )(*inputs)


def from_everyone(value, axis):
    peers = lax.axis_size(axis)
    return lax.all_to_all(jnp.broadcast_to(value[None], (peers, *value.shape)), axis, 0, 0, tiled=True)


def on_device(right_side, couplings, center, ocean_mask):
    ny, nx = lax.axis_size(GY), lax.axis_size(GX)
    is_top = (lax.axis_index(GY) == ny - 1).astype(jnp.int32).reshape(1)
    planes = jnp.concatenate([couplings, jnp.where(ocean_mask != 0, center, 0.0)[None]], axis=0)
    last = jnp.concatenate([right_side[:, -HALO:], planes[:, -HALO:]], axis=0)
    first = jnp.concatenate([right_side[:, :HALO], planes[:, :HALO]], axis=0)
    south = lax.ppermute(last, GY, [(k, k + 1) for k in range(ny - 1)])
    north = lax.ppermute(first, GY, [(k + 1, k) for k in range(ny - 1)])
    row = (ny - 1) * nx
    fold = lax.ppermute(last[:, ::-1, ::-1], ALL, [(row + k, row + nx - 1 - k) for k in range(nx)])

    packed = shape(3, TILES, 8, LANES)
    own_west, own_east, north = call(
        pack_kernel, (right_side, planes, south, north, fold), (packed, packed, shape(MEMBERS + PLANES, 8, LANES)),
        name="pack",
    )
    from_west = lax.ppermute(own_east, GX, [(k, (k + 1) % nx) for k in range(nx)])
    from_east = lax.ppermute(own_west, GX, [((k + 1) % nx, k) for k in range(nx)])

    size = 16 + MEMBERS * EXT
    basis, diag, gram = call(
        basis_kernel,
        (is_top, right_side, planes, south, north, own_west, own_east, from_west, from_east),
        (shape(BASIS, size, LANES), shape(ROWS, LANES), shape(8, LANES)),
        scratch=(
            pltpu.VMEM((ITERS, 16 + GROUPS * EXT, LANES), F32),
            pltpu.VMEM((16 + PLANES * EXT, LANES), F32),
            pltpu.VMEM((16 + PLANES * EXT, LANES), F32),
            pltpu.VMEM((TILES, 8, 8, LANES), F32),
            pltpu.VMEM((TILES, 8, 8, LANES), F32),
            pltpu.VMEM((TILES, 8, LANES), F32),
            pltpu.VMEM((TILES, 8, LANES), F32),
            pltpu.VMEM((len(PAIRS) * MEMBERS * 8, LANES), F32),
        ),
        name="basis",
        in_specs=[SMEM] + [VMEM] * 8,
    )
    parts = from_everyone(gram, GX)
    zero = jnp.zeros((8, LANES), F32)
    near = jnp.stack(sum2([(parts[k], zero) for k in range(nx)]))
    total = from_everyone(near, GY)
    return tuple(call(
        finish_kernel,
        (total, basis, diag),
        (shape(MEMBERS, ROWS, LANES), shape(MEMBERS, ROWS, LANES)),
        scratch=(pltpu.VMEM((2 * ITERS + 1, MEMBERS, LANES), F32),),
        name="finish",
    ))


def solution(mesh):
    split = Mesh(mesh.devices.reshape(8, 4, 4, 2), ("gy_0", "gy_1", "gx_0", "gx_1"))
    placed = (P(None, GY, GX), P(None, GY, GX), P(GY, GX), P(GY, GX))
    return jax.shard_map(
        on_device,
        mesh=split,
        in_specs=placed,
        out_specs=(P(None, GY, GX), P(None, GY, GX)),
        check_vma=False,
    )
```

```python
import jax
import jax.numpy as jnp
from jax import lax
from jax.experimental import pallas as pl
from jax.experimental.pallas import tpu as pltpu
from jax.sharding import Mesh
from jax.sharding import PartitionSpec as P

ITERS = 6
SHIFT = (0.375, 0.0, 0.375, 0.0, 0.375, 0.0)
GY = ("gy_0", "gy_1")
GX = ("gx_0", "gx_1")
ALL = GY + GX
NEAR = ("gy_0", "gx_1")
FAR = ("gy_1", "gx_0")
MEMBERS = 32
ROWS = 64
LANES = 128
HALO = 8
TILES = (ROWS + 2 * HALO) // 8
EXT = ROWS + 2 * HALO
GROUPS = MEMBERS // 4
PLANES = 4
BASIS = ITERS + 1
PAIRS = [(i, j) for i in range(ITERS) for j in range(i, BASIS)]
INTERPRET = False
F32 = jnp.float32
VMEM = pl.BlockSpec(memory_space=pltpu.VMEM)
SMEM = pl.BlockSpec(memory_space=pltpu.SMEM)
HBM = pl.BlockSpec(memory_space=pltpu.HBM)


def lanes_of():
    return lax.broadcasted_iota(jnp.int32, (8, LANES), 1)


def rolled(value, shift):
    shift %= LANES
    return value if shift == 0 else pltpu.roll(value, shift, 1)


SENT = 6
PACKED = MEMBERS * SENT + PLANES * 8


def edges_kernel(
    right_ref, couplings_ref, center_ref, mask_ref, planes_ref, last_ref, first_ref, rows_ref, center_row_ref, mask_row_ref, sems
):
    copies = [
        pltpu.make_async_copy(couplings_ref, planes_ref.at[pl.ds(0, 3)], sems.at[0]),
        pltpu.make_async_copy(center_ref, center_row_ref, sems.at[1]),
        pltpu.make_async_copy(mask_ref, mask_row_ref, sems.at[2]),
        pltpu.make_async_copy(right_ref.at[:, pl.ds(ROWS - 8, 8), :], rows_ref.at[0], sems.at[3]),
        pltpu.make_async_copy(right_ref.at[:, pl.ds(0, 8), :], rows_ref.at[1], sems.at[4]),
    ]
    for copy in copies:
        copy.start()
    for copy in copies:
        copy.wait()
    planes_ref[3] = jnp.where(mask_row_ref[...] != 0, center_row_ref[...], 0.0)
    for p in range(PLANES):
        base = MEMBERS * SENT + 8 * p
        last_ref[base : base + 8] = planes_ref[p, ROWS - 8 : ROWS]
        first_ref[base : base + 8] = planes_ref[p, 0:8]
    for m in range(MEMBERS):
        last_ref[SENT * m : SENT * m + SENT] = rows_ref[0, m, 8 - SENT : 8]
        first_ref[SENT * m : SENT * m + SENT] = rows_ref[1, m, 0:SENT]


def pack(load, store, west_ref, east_ref, tile):
    window = lanes_of() // 8
    for h in range(3):
        members = range(16 * h, 16 * h + 16) if h < 2 else range(MEMBERS, MEMBERS + PLANES)
        first = last = None
        for m in members:
            value = rolled(load(m), 32 * (m % 4))
            if m < MEMBERS:
                store(m, value)
            extra = 8 * (m // 4 % 4) if h < 2 else 0
            low, high = rolled(value, extra), rolled(value, extra + 8)
            if first is None:
                first, last = low, high
            else:
                here = window == 4 * (m % 4) + extra // 8
                first = jnp.where(here, low, first)
                last = jnp.where(here, high, last)
        west_ref[h, tile] = first
        east_ref[h, tile] = last


def pack_own_kernel(right_hbm_ref, planes_ref, turned_ref, west_ref, east_ref, right_ref, sem):
    copy = pltpu.make_async_copy(right_hbm_ref, right_ref, sem)
    copy.start()
    copy.wait()

    def own(t, _):
        at = pl.multiple_of(8 * t, 8)

        def load(m):
            return right_ref[m, pl.ds(at, 8), :] if m < MEMBERS else planes_ref[m - MEMBERS, pl.ds(at, 8), :]

        def store(m, value):
            turned_ref[m, pl.ds(at, 8), :] = value

        pack(load, store, west_ref, east_ref, t)
        return 0

    lax.fori_loop(0, ROWS // 8, own, 0)


def pack_halo_kernel(
    south_ref, north_ref, fold_ref, own_west_ref, own_east_ref, turned_ref, planes_ref, west_ref, east_ref, rows_ref
):
    for h in range(3):
        west_ref[h, 1 : TILES - 1] = own_west_ref[h]
        east_ref[h, 1 : TILES - 1] = own_east_ref[h]
    zero = jnp.zeros((8, LANES), F32)
    for m in range(MEMBERS):
        rows_ref[0, m] = zero
        rows_ref[1, m] = zero
        rows_ref[0, m, 8 - SENT : 8] = south_ref[SENT * m : SENT * m + SENT]
        back = PACKED - SENT * (m + 1)
        rows_ref[1, m, 0:SENT] = north_ref[SENT * m : SENT * m + SENT] + fold_ref[back : back + SENT]
    for p in range(PLANES):
        base = MEMBERS * SENT + 8 * p
        back = PACKED - base - 8
        planes_ref[p, 0] = south_ref[base : base + 8]
        planes_ref[p, 1] = north_ref[base : base + 8] + fold_ref[back : back + 8]
    for k, tile in ((0, 0), (1, TILES - 1)):
        def load(m, k=k):
            return rows_ref[k, m] if m < MEMBERS else planes_ref[m - MEMBERS, k]

        def store(m, value, k=k):
            turned_ref[m, k] = value

        pack(load, store, west_ref, east_ref, tile)


def basis_kernel(
    top_ref, right_ref, right_halo_ref, planes_ref, planes_halo_ref,
    own_west_ref, own_east_ref, from_west_ref, from_east_ref,
    basis_ref, diag_ref, gram_ref,
    strip_ref, plane_ref, plane_strip_ref, weight_ref, weight_strip_ref, inverse_ref, inverse_strip_ref,
    edge_ref, partial_ref,
):
    lane = lanes_of()
    spot = (lane + 7) % 32

    def main_row(member, tile):
        return 8 + member * EXT + 8 * tile

    def at8(row):
        return pl.ds(pl.multiple_of(row, 8), 8)

    zero = jnp.zeros((8, LANES), F32)
    for j in range(ITERS):
        basis_ref[j, 0:8] = zero
        basis_ref[j, 8 + MEMBERS * EXT : 16 + MEMBERS * EXT] = zero
        strip_ref[j, 0:8] = zero
        strip_ref[j, 8 + GROUPS * EXT : 16 + GROUPS * EXT] = zero

    for p in range(PLANES):
        base = 8 + p * EXT
        plane_ref[base : base + 8] = planes_halo_ref[p, 0]
        plane_ref[base + 8 : base + 8 + ROWS] = planes_ref[p]
        plane_ref[base + 8 + ROWS : base + EXT] = planes_halo_ref[p, 1]
    plane_ref[0:8] = zero
    plane_ref[8 + PLANES * EXT : 16 + PLANES * EXT] = zero
    plane_strip_ref[0:8] = zero
    plane_strip_ref[8 + PLANES * EXT : 16 + PLANES * EXT] = zero

    def joined(h, tile, at):
        out = rolled(from_west_ref[h, tile], -7 - at)
        out = jnp.where(spot < 8, out, rolled(own_west_ref[h, tile], 1 - at))
        out = jnp.where(spot < 16, out, rolled(own_east_ref[h, tile], 9 - at))
        return jnp.where(spot < 24, out, rolled(from_east_ref[h, tile], 17 - at))

    def plane_strips(t, _):
        value = joined(2, t, 0)
        for p in range(PLANES):
            one = jnp.where((lane + 7) // 32 % 4 == p, value, 0.0)
            one = one + pltpu.roll(one, 32, 1)
            one = one + pltpu.roll(one, 64, 1)
            plane_strip_ref[at8(8 + p * EXT + 8 * t), :] = one
        return 0

    lax.fori_loop(0, TILES, plane_strips, 0)

    def weights(t, ghost):
        dr = 1 if ghost else -1
        side = LANES - 1 if ghost else 1

        def row(ref, p, shift):
            return ref[pl.ds(8 + p * EXT + 8 * t + shift, 8), :]

        def beside(main, strip):
            if ghost:
                return jnp.where(lane == LANES - 1, pltpu.roll(strip, 110, 1), pltpu.roll(main, side, 1))
            return jnp.where(lane == 0, strip, pltpu.roll(main, side, 1))

        def finish(cn0, cnr, ce0, cec, cc0, ccr, ccc, ccrc, center, main):
            total = center + cn0 + cnr + ce0 + cec + cc0 + ccr + ccc + ccrc
            inv = jnp.where(center > 0.0, 1.0 / total, 0.0)
            if ghost:
                w = dict(s=cn0, n=cnr, w=ce0, e=cec, sw=cc0, nw=ccr, se=ccc, ne=ccrc)
            else:
                w = dict(n=cn0, s=cnr, e=ce0, w=cec, ne=cc0, se=ccr, nw=ccc, sw=ccrc)

            def ahead(value):
                value = pltpu.roll(value * inv, 1, 1)
                return jnp.where(lane == 0, 0.0, value) if main else value

            def behind(value):
                value = pltpu.roll(value * inv, LANES - 1, 1)
                return jnp.where(lane == LANES - 1, 0.0, value) if main else value

            return total, inv, (
                w["s"] * inv, w["n"] * inv,
                ahead(w["se"]), ahead(w["e"]), ahead(w["ne"]),
                behind(w["sw"]), behind(w["w"]), behind(w["nw"]),
            )

        strips = [row(plane_strip_ref, p, 0) for p in range(PLANES)]
        strips_r = [row(plane_strip_ref, p, dr) for p in (0, 2)]
        _, inv, ws = finish(
            strips[0], strips_r[0], strips[1], pltpu.roll(strips[1], side, 1),
            strips[2], strips_r[1], pltpu.roll(strips[2], side, 1), pltpu.roll(strips_r[1], side, 1),
            strips[3], False,
        )
        inverse_strip_ref[t] = inv
        for k in range(8):
            weight_strip_ref[t, k] = ws[k]
        mains = [row(plane_ref, p, 0) for p in range(PLANES)]
        mains_r = [row(plane_ref, p, dr) for p in (0, 2)]
        total, inv, ws = finish(
            mains[0], mains_r[0], mains[1], beside(mains[1], strips[1]),
            mains[2], mains_r[1], beside(mains[2], strips[2]), beside(mains_r[1], strips_r[1]),
            mains[3], True,
        )
        for q in range(4):
            inverse_ref[t, q] = rolled(inv, 32 * q)
            for k in range(8):
                weight_ref[t, q, k] = rolled(ws[k], 32 * q)
        return total

    weights(0, False)

    def inner_weights(t, _):
        total = weights(t, False)
        for q in range(4):
            diag_ref[q, at8(8 * (t - 1)), :] = rolled(total, 32 * q)
        return 0

    lax.fori_loop(1, TILES - 1, inner_weights, 0)

    @pl.when(top_ref[0] == 0)
    def _():
        weights(TILES - 1, False)

    @pl.when(top_ref[0] != 0)
    def _():
        weights(TILES - 1, True)

    def first(t, load):
        for q in range(4):
            inv = inverse_ref[t, q]
            for s in range(GROUPS):
                m = 4 * s + q
                basis_ref[0, at8(main_row(m, t)), :] = load(m) * inv
        inv = inverse_strip_ref[t]
        for s in range(GROUPS):
            strip_ref[0, at8(8 + s * EXT + 8 * t), :] = joined(s // 4, t, 8 * (s % 4)) * inv

    first(0, lambda m: right_halo_ref[m, 0])

    def inner_first(t, _):
        first(t, lambda m: right_ref[m, at8(8 * (t - 1)), :])
        return 0

    lax.fori_loop(1, TILES - 1, inner_first, 0)
    first(TILES - 1, lambda m: right_halo_ref[m, 1])

    def parts(ref, j, base, w):
        a = ref[j, pl.ds(base - 1, 8), :]
        b = ref[j, at8(base), :]
        c = ref[j, pl.ds(base + 1, 8), :]
        middle = w[0] * a + w[1] * c
        if SHIFT[j]:
            middle = middle - SHIFT[j] * b
        return middle, (w[2] * a + w[4] * c) + w[3] * b, (w[5] * a + w[7] * c) + w[6] * b

    one = top_ref[1]

    def staged(work):
        waiting = []
        for begin, end in work:
            waiting.append((end, begin()))
            if len(waiting) > 2:
                end, values = waiting.pop(0)
                end(values)
        for end, values in waiting:
            end(values)

    def strip_work(j, t):
        def begin():
            w = [weight_strip_ref[t, k] for k in range(8)]
            values = []
            for s in range(GROUPS):
                middle, ahead, behind = parts(strip_ref, j, 8 + s * EXT + 8 * t, w)
                edge = jnp.where(lane % 32 == 31, pltpu.roll(ahead, LANES - 18, 1), behind)
                moved = (pltpu.roll(ahead, LANES - 1, 1), pltpu.roll(behind, 1, 1)) if j + 1 < ITERS else ()
                values.append((middle, edge, moved))
            return values

        def end(values):
            for s, (middle, edge, moved) in enumerate(values):
                edge_ref[t, s] = edge
                if moved:
                    strip_ref[j + one, at8(8 + s * EXT + 8 * t), :] = middle + moved[0] + moved[1]

        return begin, end

    def main_work(j, t, q, groups):
        def begin():
            w = [weight_ref[t, q, k] for k in range(8)]
            ends = (lane == 32 * q) | (lane == (32 * q - 1) % LANES)
            values = []
            for s in groups:
                middle, ahead, behind = parts(basis_ref, j, main_row(4 * s + q, t), w)
                middle = middle + jnp.where(ends, edge_ref[t, s], 0.0)
                values.append((middle, pltpu.roll(ahead, LANES - 1, 1), pltpu.roll(behind, 1, 1)))
            return values

        def end(values):
            for s, (middle, ahead, behind) in zip(groups, values):
                basis_ref[j + one, at8(main_row(4 * s + q, t)), :] = middle + ahead + behind

        return begin, end

    for j in range(ITERS):
        low, high = (0, TILES) if j + 1 < ITERS else (1, TILES - 1)
        half = (high - low) // 2

        def strip_body(n, _, j=j, low=low, half=half):
            staged([strip_work(j, low + half * n + k) for k in range(half)])
            return 0

        def main_body(n, _, j=j, low=low):
            staged([
                main_work(j, low + 2 * n + k, q, range(g, g + 8))
                for k in range(2) for q in range(4) for g in range(0, GROUPS, 8)
            ])
            return 0

        lax.fori_loop(0, 2, strip_body, 0)
        lax.fori_loop(0, (high - low) // 2, main_body, 0)

    def products(s, _):
        for q in range(4):
            m = 4 * s + q
            sums = [None] * len(PAIRS)
            for t in range(1, TILES - 1):
                u = [basis_ref[j, at8(main_row(m, t)), :] for j in range(BASIS)]
                d = diag_ref[q, 8 * (t - 1) : 8 * t]
                scaled = [d * u[j] for j in range(ITERS)]
                for n, (i, j) in enumerate(PAIRS):
                    term = scaled[i] * u[j]
                    sums[n] = term if sums[n] is None else sums[n] + term
            for n in range(len(PAIRS)):
                partial_ref[at8((n * MEMBERS + m) * 8), :] = sums[n]
        return 0

    lax.fori_loop(0, GROUPS, products, 0)
    result = zero
    for l in range(len(PAIRS) * MEMBERS // 8):
        rows = [partial_ref[pl.ds(64 * l + k, 8, stride=8), :] for k in range(8)]
        while len(rows) > 1:
            rows = [rows[k] + rows[k + 1] for k in range(0, len(rows), 2)]
        result = jnp.where(lane == l, jnp.sum(rows[0], axis=1, keepdims=True), result)
    for n in range(gram_ref.shape[0]):
        gram_ref[n] = result


def two_sum(a, b):
    s = a + b
    t = s - a
    return s, (a - (s - t)) + (b - t)


def quick(a, b):
    s = a + b
    return s, b - (s - a)


def halves(a):
    t = 4097.0 * a
    high = t - (t - a)
    return high, a - high


def add2(a, b):
    s, e = two_sum(a[0], b[0])
    return quick(s, e + (a[1] + b[1]))


def mul2(a, b):
    p = a[0] * b[0]
    ah, al = halves(a[0])
    bh, bl = halves(b[0])
    e = ((ah * bh - p) + ah * bl + al * bh) + al * bl
    return quick(p, e + (a[0] * b[1] + a[1] * b[0]))


def neg2(a):
    return -a[0], -a[1]


def div2(a, b):
    q = a[0] / b[0]
    zero = jnp.zeros_like(q)
    rest = add2(a, neg2(mul2((q, zero), b)))
    return quick(q, rest[0] / b[0])


def sum2(terms):
    terms = list(terms)
    while len(terms) > 1:
        terms = [add2(terms[k], terms[k + 1]) if k + 1 < len(terms) else terms[k] for k in range(0, len(terms), 2)]
    return terms[0]


def finish_kernel(total_ref, basis_ref, diag_ref, solved_ref, left_ref, coeff_ref, solution_ref, residual_ref, sems):
    count = total_ref.shape[0]
    high, low = sum2([(total_ref[n, 0], total_ref[n, 1]) for n in range(count)])
    gram = {}
    for n, (i, j) in enumerate(PAIRS):
        shift = (LANES - 4 * n) % LANES
        value = (high, low) if shift == 0 else (pltpu.roll(high, shift, 1), pltpu.roll(low, shift, 1))
        gram[i, j] = gram[j, i] = value

    def scaled(value, factor):
        if factor == 1.0:
            return value
        s, e = two_sum(0.5 * value[0], 0.125 * value[0])
        return quick(s, e + factor * value[1])

    def dot(a, b):
        return sum2([mul2(x, y) for x, y in zip(a, b)])

    one = (jnp.ones((8, LANES), F32), jnp.zeros((8, LANES), F32))
    precond, direction, answer = [one], [one], []
    rz = gram[0, 0]
    for k in range(ITERS):
        image = [scaled(c, 1.0 - SHIFT[j]) for j, c in enumerate(direction)]
        image = [image[0]] + [
            add2(image[j], neg2(direction[j - 1])) for j in range(1, k + 1)
        ] + [neg2(direction[k])]
        final = k + 1 == ITERS
        row = [dot([gram[i, j] for j in range(k + 2)], image) for i in range(k + 1 if final else k + 2)]
        step_size = div2(rz, dot(direction, row))
        moved = [mul2(step_size, c) for c in direction]
        answer = [add2(a, b) for a, b in zip(answer, moved)] + moved[len(answer):]
        if not final:
            cross = dot(precond, row)
            rz_new = mul2(step_size, add2(mul2(step_size, dot(image, row)), (-2.0 * cross[0], -2.0 * cross[1])))
            rz_new = add2(rz, rz_new)
        moved = [neg2(mul2(step_size, c)) for c in image]
        precond = [add2(a, b) for a, b in zip(precond, moved)] + moved[len(precond):]
        if not final:
            ratio = div2(rz_new, rz)
            moved = [mul2(ratio, c) for c in direction]
            direction = [add2(a, b) for a, b in zip(precond, moved)] + precond[len(moved):]
            rz = rz_new

    values = [c[0] for c in answer] + [c[0] for c in precond]
    for n, value in enumerate(values):
        for l in range(MEMBERS // 8):
            coeff_ref[n, 8 * l : 8 * l + 8] = jnp.broadcast_to(value[:, l : l + 1], (8, LANES))

    def combine(s, _):
        for q in range(4):
            m = 4 * s + q
            c = [jnp.broadcast_to(coeff_ref[n, pl.ds(m, 1), :], (8, LANES)) for n in range(2 * ITERS + 1)]
            for t in range(ROWS // 8):
                at = pl.multiple_of(16 + m * EXT + 8 * t, 8)
                u = [basis_ref[j, pl.ds(at, 8), :] for j in range(BASIS)]
                solved = c[0] * u[0]
                left = c[ITERS] * u[0]
                for j in range(1, BASIS):
                    if j < ITERS:
                        solved = solved + c[j] * u[j]
                    left = left + c[ITERS + j] * u[j]
                solution_ref[m, 8 * t : 8 * t + 8] = rolled(solved, -32 * q)
                residual_ref[m, 8 * t : 8 * t + 8] = rolled(diag_ref[q, 8 * t : 8 * t + 8] * left, -32 * q)
        for copy in copies(s):
            copy.start()
        return 0

    def copies(s):
        members = pl.ds(4 * s, 4)
        return [
            pltpu.make_async_copy(source.at[members], target.at[members], sems.at[n, s])
            for n, (source, target) in enumerate(((solution_ref, solved_ref), (residual_ref, left_ref)))
        ]

    lax.fori_loop(0, GROUPS, combine, 0)
    for s in range(GROUPS):
        for copy in copies(s):
            copy.wait()


def shape(*dims):
    return jax.ShapeDtypeStruct(dims, F32)


def call(kernel, inputs, out_shape, scratch=(), name=None, in_specs=None, out_specs=None):
    return pl.pallas_call(
        kernel,
        out_shape=out_shape,
        in_specs=in_specs or [VMEM] * len(inputs),
        out_specs=out_specs or [VMEM] * len(out_shape),
        scratch_shapes=list(scratch),
        interpret=INTERPRET,
        name=name,
        compiler_params=pltpu.CompilerParams(vmem_limit_bytes=28 * 1024 * 1024),
    )(*inputs)


def on_device(right_side, couplings, center, ocean_mask):
    ny, nx = lax.axis_size(GY), lax.axis_size(GX)
    top = jnp.stack([(lax.axis_index(GY) == ny - 1).astype(jnp.int32), jnp.int32(1)])
    sent = shape(PACKED, LANES)
    right_side, couplings, center, ocean_mask = (
        pltpu.with_memory_space_constraint(a, pltpu.HBM) for a in (right_side, couplings, center, ocean_mask)
    )
    planes, last, first = call(
        edges_kernel, (right_side, couplings, center, ocean_mask), (shape(PLANES, ROWS, LANES), sent, sent),
        scratch=(
            pltpu.VMEM((2, MEMBERS, 8, LANES), F32),
            pltpu.VMEM((ROWS, LANES), F32),
            pltpu.VMEM((ROWS, LANES), jnp.int32),
            pltpu.SemaphoreType.DMA((5,)),
        ),
        name="edges",
        in_specs=[HBM] * 4,
    )
    with jax.named_scope("south"):
        south = lax.ppermute(last, GY, [(k, k + 1) for k in range(ny - 1)])
    with jax.named_scope("north"):
        north = lax.ppermute(first, GY, [(k + 1, k) for k in range(ny - 1)])
    row = (ny - 1) * nx
    turned_last = last[::-1, ::-1]
    with jax.named_scope("fold"):
        fold = lax.ppermute(turned_last, ALL, [(row + k, row + nx - 1 - k) for k in range(nx)])

    inner = shape(3, TILES - 2, 8, LANES)
    turned, inner_west, inner_east = call(
        pack_own_kernel, (right_side, planes), (shape(MEMBERS, ROWS, LANES), inner, inner), name="pack_own",
        scratch=(pltpu.VMEM((MEMBERS, ROWS, LANES), F32), pltpu.SemaphoreType.DMA),
        in_specs=[HBM, VMEM],
    )
    packed = shape(3, TILES, 8, LANES)
    turned_halo, planes_halo, own_west, own_east = call(
        pack_halo_kernel,
        (south, north, fold, inner_west, inner_east),
        (shape(MEMBERS, 2, 8, LANES), shape(PLANES, 2, 8, LANES), packed, packed),
        scratch=(pltpu.VMEM((2, MEMBERS, 8, LANES), F32),),
        name="pack_halo",
    )
    from_west = lax.ppermute(own_east, GX, [(k, (k + 1) % nx) for k in range(nx)])
    from_east = lax.ppermute(own_west, GX, [((k + 1) % nx, k) for k in range(nx)])

    near, far = lax.axis_size(NEAR), lax.axis_size(FAR)
    basis, diag, gram = call(
        basis_kernel,
        (top, turned, turned_halo, planes, planes_halo, own_west, own_east, from_west, from_east),
        (shape(BASIS, 16 + MEMBERS * EXT, LANES), shape(4, ROWS, LANES), shape(near, 8, LANES)),
        scratch=(
            pltpu.VMEM((ITERS, 16 + GROUPS * EXT, LANES), F32),
            pltpu.VMEM((16 + PLANES * EXT, LANES), F32),
            pltpu.VMEM((16 + PLANES * EXT, LANES), F32),
            pltpu.VMEM((TILES, 4, 8, 8, LANES), F32),
            pltpu.VMEM((TILES, 8, 8, LANES), F32),
            pltpu.VMEM((TILES, 4, 8, LANES), F32),
            pltpu.VMEM((TILES, 8, LANES), F32),
            pltpu.VMEM((TILES, GROUPS, 8, LANES), F32),
            pltpu.VMEM((len(PAIRS) * MEMBERS * 8, LANES), F32),
        ),
        name="basis",
        in_specs=[SMEM] + [VMEM] * 8,
    )
    parts = lax.all_to_all(gram, NEAR, 0, 0, tiled=True)
    zero = jnp.zeros((8, LANES), F32)
    mine = jnp.stack(sum2([(parts[k], zero) for k in range(near)]))
    total = lax.all_to_all(jnp.broadcast_to(mine[None], (far, *mine.shape)), FAR, 0, 0, tiled=True)
    return tuple(call(
        finish_kernel,
        (total, basis, diag),
        (shape(MEMBERS, ROWS, LANES), shape(MEMBERS, ROWS, LANES)),
        scratch=(
            pltpu.VMEM((2 * ITERS + 1, MEMBERS, LANES), F32),
            pltpu.VMEM((MEMBERS, ROWS, LANES), F32),
            pltpu.VMEM((MEMBERS, ROWS, LANES), F32),
            pltpu.SemaphoreType.DMA((2, GROUPS)),
        ),
        name="finish",
        out_specs=[HBM, HBM],
    ))


def solution(mesh):
    split = Mesh(mesh.devices.reshape(8, 4, 4, 2), ("gy_0", "gy_1", "gx_0", "gx_1"))
    placed = (P(None, GY, GX), P(None, GY, GX), P(GY, GX), P(GY, GX))
    return jax.shard_map(
        on_device,
        mesh=split,
        in_specs=placed,
        out_specs=(P(None, GY, GX), P(None, GY, GX)),
        check_vma=False,
    )
```

```python
import jax
import jax.numpy as jnp
from jax import lax
from jax.experimental import pallas as pl
from jax.experimental.pallas import tpu as pltpu
from jax.sharding import Mesh
from jax.sharding import PartitionSpec as P

ITERS = 6
SHIFT = (0.375, 0.0, 0.375, 0.0, 0.375, 0.0)
GY = ("gy_0", "gy_1")
GX = ("gx_0", "gx_1")
ALL = GY + GX
NEAR = ("gy_0", "gx_1")
FAR = ("gy_1", "gx_0")
MEMBERS = 32
ROWS = 64
LANES = 128
HALO = 8
TILES = (ROWS + 2 * HALO) // 8
EXT = ROWS + 2 * HALO
GROUPS = MEMBERS // 4
PLANES = 4
BASIS = ITERS + 1
PAIRS = [(i, j) for i in range(ITERS) for j in range(i, BASIS)]
INTERPRET = False
F32 = jnp.float32
VMEM = pl.BlockSpec(memory_space=pltpu.VMEM)
SMEM = pl.BlockSpec(memory_space=pltpu.SMEM)
HBM = pl.BlockSpec(memory_space=pltpu.HBM)


def lanes_of():
    return lax.broadcasted_iota(jnp.int32, (8, LANES), 1)


def rolled(value, shift):
    shift %= LANES
    return value if shift == 0 else pltpu.roll(value, shift, 1)


SENT = 6
PACKED = MEMBERS * SENT + PLANES * 8


def edges_kernel(
    right_ref, couplings_ref, center_ref, mask_ref, planes_ref, last_ref, first_ref, rows_ref, center_row_ref, mask_row_ref, sems
):
    copies = [
        pltpu.make_async_copy(couplings_ref, planes_ref.at[pl.ds(0, 3)], sems.at[0]),
        pltpu.make_async_copy(center_ref, center_row_ref, sems.at[1]),
        pltpu.make_async_copy(mask_ref, mask_row_ref, sems.at[2]),
        pltpu.make_async_copy(right_ref.at[:, pl.ds(ROWS - 8, 8), :], rows_ref.at[0], sems.at[3]),
        pltpu.make_async_copy(right_ref.at[:, pl.ds(0, 8), :], rows_ref.at[1], sems.at[4]),
    ]
    for copy in copies:
        copy.start()
    for copy in copies:
        copy.wait()
    planes_ref[3] = jnp.where(mask_row_ref[...] != 0, center_row_ref[...], 0.0)
    for p in range(PLANES):
        base = MEMBERS * SENT + 8 * p
        last_ref[base : base + 8] = planes_ref[p, ROWS - 8 : ROWS]
        first_ref[base : base + 8] = planes_ref[p, 0:8]
    for m in range(MEMBERS):
        last_ref[SENT * m : SENT * m + SENT] = rows_ref[0, m, 8 - SENT : 8]
        first_ref[SENT * m : SENT * m + SENT] = rows_ref[1, m, 0:SENT]


def pack(load, store, west_ref, east_ref, tile):
    window = lanes_of() // 8
    for h in range(3):
        members = range(16 * h, 16 * h + 16) if h < 2 else range(MEMBERS, MEMBERS + PLANES)
        first = last = None
        for m in members:
            value = rolled(load(m), 32 * (m % 4))
            if m < MEMBERS:
                store(m, value)
            extra = 8 * (m // 4 % 4) if h < 2 else 0
            low, high = rolled(value, extra), rolled(value, extra + 8)
            if first is None:
                first, last = low, high
            else:
                here = window == 4 * (m % 4) + extra // 8
                first = jnp.where(here, low, first)
                last = jnp.where(here, high, last)
        west_ref[h, tile] = first
        east_ref[h, tile] = last


def pack_own_kernel(right_hbm_ref, planes_ref, turned_ref, west_ref, east_ref, right_ref, sem):
    copy = pltpu.make_async_copy(right_hbm_ref, right_ref, sem)
    copy.start()
    copy.wait()

    def own(t, _):
        at = pl.multiple_of(8 * t, 8)

        def load(m):
            return right_ref[m, pl.ds(at, 8), :] if m < MEMBERS else planes_ref[m - MEMBERS, pl.ds(at, 8), :]

        def store(m, value):
            turned_ref[m, pl.ds(at, 8), :] = value

        pack(load, store, west_ref, east_ref, t)
        return 0

    lax.fori_loop(0, ROWS // 8, own, 0)


def pack_halo_kernel(
    south_ref, north_ref, fold_ref, own_west_ref, own_east_ref, turned_ref, planes_ref, west_ref, east_ref, rows_ref
):
    for h in range(3):
        west_ref[h, 1 : TILES - 1] = own_west_ref[h]
        east_ref[h, 1 : TILES - 1] = own_east_ref[h]
    zero = jnp.zeros((8, LANES), F32)
    for m in range(MEMBERS):
        rows_ref[0, m] = zero
        rows_ref[1, m] = zero
        rows_ref[0, m, 8 - SENT : 8] = south_ref[SENT * m : SENT * m + SENT]
        back = PACKED - SENT * (m + 1)
        rows_ref[1, m, 0:SENT] = north_ref[SENT * m : SENT * m + SENT] + fold_ref[back : back + SENT]
    for p in range(PLANES):
        base = MEMBERS * SENT + 8 * p
        back = PACKED - base - 8
        planes_ref[p, 0] = south_ref[base : base + 8]
        planes_ref[p, 1] = north_ref[base : base + 8] + fold_ref[back : back + 8]
    for k, tile in ((0, 0), (1, TILES - 1)):
        def load(m, k=k):
            return rows_ref[k, m] if m < MEMBERS else planes_ref[m - MEMBERS, k]

        def store(m, value, k=k):
            turned_ref[m, k] = value

        pack(load, store, west_ref, east_ref, tile)


def basis_kernel(
    top_ref, right_ref, right_halo_ref, planes_ref, planes_halo_ref,
    own_west_ref, own_east_ref, from_west_ref, from_east_ref,
    basis_ref, diag_ref, gram_ref,
    strip_ref, plane_ref, plane_strip_ref, weight_ref, weight_strip_ref, inverse_ref, inverse_strip_ref,
    edge_ref, partial_ref,
):
    lane = lanes_of()
    spot = (lane + 7) % 32

    def main_row(member, tile):
        return 8 + member * EXT + 8 * tile

    def at8(row):
        return pl.ds(pl.multiple_of(row, 8), 8)

    zero = jnp.zeros((8, LANES), F32)
    for j in range(ITERS):
        basis_ref[j, 0:8] = zero
        basis_ref[j, 8 + MEMBERS * EXT : 16 + MEMBERS * EXT] = zero
        strip_ref[j, 0:8] = zero
        strip_ref[j, 8 + GROUPS * EXT : 16 + GROUPS * EXT] = zero

    for p in range(PLANES):
        base = 8 + p * EXT
        plane_ref[base : base + 8] = planes_halo_ref[p, 0]
        plane_ref[base + 8 : base + 8 + ROWS] = planes_ref[p]
        plane_ref[base + 8 + ROWS : base + EXT] = planes_halo_ref[p, 1]
    plane_ref[0:8] = zero
    plane_ref[8 + PLANES * EXT : 16 + PLANES * EXT] = zero
    plane_strip_ref[0:8] = zero
    plane_strip_ref[8 + PLANES * EXT : 16 + PLANES * EXT] = zero

    def joined(h, tile, at):
        out = rolled(from_west_ref[h, tile], -7 - at)
        out = jnp.where(spot < 8, out, rolled(own_west_ref[h, tile], 1 - at))
        out = jnp.where(spot < 16, out, rolled(own_east_ref[h, tile], 9 - at))
        return jnp.where(spot < 24, out, rolled(from_east_ref[h, tile], 17 - at))

    def plane_strips(t, _):
        value = joined(2, t, 0)
        for p in range(PLANES):
            one = jnp.where((lane + 7) // 32 % 4 == p, value, 0.0)
            one = one + pltpu.roll(one, 32, 1)
            one = one + pltpu.roll(one, 64, 1)
            plane_strip_ref[at8(8 + p * EXT + 8 * t), :] = one
        return 0

    lax.fori_loop(0, TILES, plane_strips, 0, unroll=True)

    def weights(t, ghost):
        dr = 1 if ghost else -1
        side = LANES - 1 if ghost else 1

        def row(ref, p, shift):
            return ref[pl.ds(8 + p * EXT + 8 * t + shift, 8), :]

        def beside(main, strip):
            if ghost:
                return jnp.where(lane == LANES - 1, pltpu.roll(strip, 110, 1), pltpu.roll(main, side, 1))
            return jnp.where(lane == 0, strip, pltpu.roll(main, side, 1))

        def finish(cn0, cnr, ce0, cec, cc0, ccr, ccc, ccrc, center, main):
            total = center + cn0 + cnr + ce0 + cec + cc0 + ccr + ccc + ccrc
            inv = jnp.where(center > 0.0, 1.0 / total, 0.0)
            if ghost:
                w = dict(s=cn0, n=cnr, w=ce0, e=cec, sw=cc0, nw=ccr, se=ccc, ne=ccrc)
            else:
                w = dict(n=cn0, s=cnr, e=ce0, w=cec, ne=cc0, se=ccr, nw=ccc, sw=ccrc)

            def ahead(value):
                value = pltpu.roll(value * inv, 1, 1)
                return jnp.where(lane == 0, 0.0, value) if main else value

            def behind(value):
                value = pltpu.roll(value * inv, LANES - 1, 1)
                return jnp.where(lane == LANES - 1, 0.0, value) if main else value

            return total, inv, (
                w["s"] * inv, w["n"] * inv,
                ahead(w["se"]), ahead(w["e"]), ahead(w["ne"]),
                behind(w["sw"]), behind(w["w"]), behind(w["nw"]),
            )

        strips = [row(plane_strip_ref, p, 0) for p in range(PLANES)]
        strips_r = [row(plane_strip_ref, p, dr) for p in (0, 2)]
        _, inv, ws = finish(
            strips[0], strips_r[0], strips[1], pltpu.roll(strips[1], side, 1),
            strips[2], strips_r[1], pltpu.roll(strips[2], side, 1), pltpu.roll(strips_r[1], side, 1),
            strips[3], False,
        )
        inverse_strip_ref[t] = inv
        for k in range(8):
            weight_strip_ref[t, k] = ws[k]
        mains = [row(plane_ref, p, 0) for p in range(PLANES)]
        mains_r = [row(plane_ref, p, dr) for p in (0, 2)]
        total, inv, ws = finish(
            mains[0], mains_r[0], mains[1], beside(mains[1], strips[1]),
            mains[2], mains_r[1], beside(mains[2], strips[2]), beside(mains_r[1], strips_r[1]),
            mains[3], True,
        )
        for q in range(4):
            inverse_ref[t, q] = rolled(inv, 32 * q)
            for k in range(8):
                weight_ref[t, q, k] = rolled(ws[k], 32 * q)
        return total

    weights(0, False)

    def inner_weights(t, _):
        total = weights(t, False)
        for q in range(4):
            diag_ref[q, at8(8 * (t - 1)), :] = rolled(total, 32 * q)
        return 0

    lax.fori_loop(1, TILES - 1, inner_weights, 0, unroll=4)

    @pl.when(top_ref[0] == 0)
    def _():
        weights(TILES - 1, False)

    @pl.when(top_ref[0] != 0)
    def _():
        weights(TILES - 1, True)

    def first(t, load):
        for q in range(4):
            inv = inverse_ref[t, q]
            for s in range(GROUPS):
                m = 4 * s + q
                basis_ref[0, at8(main_row(m, t)), :] = load(m) * inv
        inv = inverse_strip_ref[t]
        for s in range(GROUPS):
            strip_ref[0, at8(8 + s * EXT + 8 * t), :] = joined(s // 4, t, 8 * (s % 4)) * inv

    first(0, lambda m: right_halo_ref[m, 0])

    def inner_first(t, _):
        first(t, lambda m: right_ref[m, at8(8 * (t - 1)), :])
        return 0

    lax.fori_loop(1, TILES - 1, inner_first, 0, unroll=4)
    first(TILES - 1, lambda m: right_halo_ref[m, 1])

    def parts(ref, j, base, w):
        a = ref[j, pl.ds(base - 1, 8), :]
        b = ref[j, at8(base), :]
        c = ref[j, pl.ds(base + 1, 8), :]
        middle = w[0] * a + w[1] * c
        if SHIFT[j]:
            middle = middle - SHIFT[j] * b
        return middle, (w[2] * a + w[4] * c) + w[3] * b, (w[5] * a + w[7] * c) + w[6] * b

    def staged(work):
        begun = [(end, begin()) for begin, end in work]
        for end, values in begun:
            end(values)

    def strip_work(j, t):
        def begin():
            w = [weight_strip_ref[t, k] for k in range(8)]
            values = []
            for s in range(GROUPS):
                middle, ahead, behind = parts(strip_ref, j, 8 + s * EXT + 8 * t, w)
                edge = jnp.where(lane % 32 == 31, pltpu.roll(ahead, LANES - 18, 1), behind)
                moved = (pltpu.roll(ahead, LANES - 1, 1), pltpu.roll(behind, 1, 1)) if j + 1 < ITERS else ()
                values.append((middle, edge, moved))
            return values

        def end(values):
            for s, (middle, edge, moved) in enumerate(values):
                edge_ref[t, s] = edge
                if moved:
                    strip_ref[j + 1, at8(8 + s * EXT + 8 * t), :] = middle + moved[0] + moved[1]

        return begin, end

    def main_work(j, t, q, groups):
        def begin():
            w = [weight_ref[t, q, k] for k in range(8)]
            ends = (lane == 32 * q) | (lane == (32 * q - 1) % LANES)
            values = []
            for s in groups:
                middle, ahead, behind = parts(basis_ref, j, main_row(4 * s + q, t), w)
                middle = middle + jnp.where(ends, edge_ref[t, s], 0.0)
                values.append((middle, pltpu.roll(ahead, LANES - 1, 1), pltpu.roll(behind, 1, 1)))
            return values

        def end(values):
            for s, (middle, ahead, behind) in zip(groups, values):
                basis_ref[j + 1, at8(main_row(4 * s + q, t)), :] = middle + ahead + behind

        return begin, end

    for j in range(ITERS):
        low, high = (0, TILES) if j + 1 < ITERS else (1, TILES - 1)
        half = (high - low) // 2

        def strip_body(n, _, j=j, low=low, half=half):
            staged([strip_work(j, low + half * n + k) for k in range(half)])
            return 0

        def main_body(n, _, j=j, low=low, half=half):
            staged([main_work(j, low + half * n + k, q, range(GROUPS)) for k in range(half) for q in range(4)])
            return 0

        lax.fori_loop(0, 2, strip_body, 0)
        lax.fori_loop(0, 2, main_body, 0)

    def products(s, _):
        for q in range(4):
            m = 4 * s + q
            sums = [None] * len(PAIRS)
            for t in range(1, TILES - 1):
                u = [basis_ref[j, at8(main_row(m, t)), :] for j in range(BASIS)]
                d = diag_ref[q, 8 * (t - 1) : 8 * t]
                scaled = [d * u[j] for j in range(ITERS)]
                for n, (i, j) in enumerate(PAIRS):
                    term = scaled[i] * u[j]
                    sums[n] = term if sums[n] is None else sums[n] + term
            for n in range(len(PAIRS)):
                partial_ref[at8((n * MEMBERS + m) * 8), :] = sums[n]
        return 0

    lax.fori_loop(0, GROUPS, products, 0)
    result = zero
    for l in range(len(PAIRS) * MEMBERS // 8):
        rows = [partial_ref[pl.ds(64 * l + k, 8, stride=8), :] for k in range(8)]
        while len(rows) > 1:
            rows = [rows[k] + rows[k + 1] for k in range(0, len(rows), 2)]
        result = jnp.where(lane == l, jnp.sum(rows[0], axis=1, keepdims=True), result)
    for n in range(gram_ref.shape[0]):
        gram_ref[n] = result


def two_sum(a, b):
    s = a + b
    t = s - a
    return s, (a - (s - t)) + (b - t)


def quick(a, b):
    s = a + b
    return s, b - (s - a)


def halves(a):
    t = 4097.0 * a
    high = t - (t - a)
    return high, a - high


def add2(a, b):
    s, e = two_sum(a[0], b[0])
    return quick(s, e + (a[1] + b[1]))


def mul2(a, b):
    p = a[0] * b[0]
    ah, al = halves(a[0])
    bh, bl = halves(b[0])
    e = ((ah * bh - p) + ah * bl + al * bh) + al * bl
    return quick(p, e + (a[0] * b[1] + a[1] * b[0]))


def neg2(a):
    return -a[0], -a[1]


def div2(a, b):
    q = a[0] / b[0]
    zero = jnp.zeros_like(q)
    rest = add2(a, neg2(mul2((q, zero), b)))
    return quick(q, rest[0] / b[0])


def sum2(terms):
    terms = list(terms)
    while len(terms) > 1:
        terms = [add2(terms[k], terms[k + 1]) if k + 1 < len(terms) else terms[k] for k in range(0, len(terms), 2)]
    return terms[0]


def finish_kernel(total_ref, basis_ref, diag_ref, solved_ref, left_ref, coeff_ref, solution_ref, residual_ref, sems):
    count = total_ref.shape[0]
    high, low = sum2([(total_ref[n, 0], total_ref[n, 1]) for n in range(count)])
    gram = {}
    for n, (i, j) in enumerate(PAIRS):
        shift = (LANES - 4 * n) % LANES
        value = (high, low) if shift == 0 else (pltpu.roll(high, shift, 1), pltpu.roll(low, shift, 1))
        gram[i, j] = gram[j, i] = value

    def scaled(value, factor):
        if factor == 1.0:
            return value
        s, e = two_sum(0.5 * value[0], 0.125 * value[0])
        return quick(s, e + factor * value[1])

    def dot(a, b):
        return sum2([mul2(x, y) for x, y in zip(a, b)])

    one = (jnp.ones((8, LANES), F32), jnp.zeros((8, LANES), F32))
    precond, direction, answer = [one], [one], []
    rz = gram[0, 0]
    for k in range(ITERS):
        image = [scaled(c, 1.0 - SHIFT[j]) for j, c in enumerate(direction)]
        image = [image[0]] + [
            add2(image[j], neg2(direction[j - 1])) for j in range(1, k + 1)
        ] + [neg2(direction[k])]
        final = k + 1 == ITERS
        row = [dot([gram[i, j] for j in range(k + 2)], image) for i in range(k + 1 if final else k + 2)]
        step_size = div2(rz, dot(direction, row))
        moved = [mul2(step_size, c) for c in direction]
        answer = [add2(a, b) for a, b in zip(answer, moved)] + moved[len(answer):]
        if not final:
            cross = dot(precond, row)
            rz_new = mul2(step_size, add2(mul2(step_size, dot(image, row)), (-2.0 * cross[0], -2.0 * cross[1])))
            rz_new = add2(rz, rz_new)
        moved = [neg2(mul2(step_size, c)) for c in image]
        precond = [add2(a, b) for a, b in zip(precond, moved)] + moved[len(precond):]
        if not final:
            ratio = div2(rz_new, rz)
            moved = [mul2(ratio, c) for c in direction]
            direction = [add2(a, b) for a, b in zip(precond, moved)] + precond[len(moved):]
            rz = rz_new

    values = [c[0] for c in answer] + [c[0] for c in precond]
    for n, value in enumerate(values):
        for l in range(MEMBERS // 8):
            coeff_ref[n, 8 * l : 8 * l + 8] = jnp.broadcast_to(value[:, l : l + 1], (8, LANES))

    def combine(s, _):
        for q in range(4):
            m = 4 * s + q
            c = [jnp.broadcast_to(coeff_ref[n, pl.ds(m, 1), :], (8, LANES)) for n in range(2 * ITERS + 1)]
            for t in range(ROWS // 8):
                at = pl.multiple_of(16 + m * EXT + 8 * t, 8)
                u = [basis_ref[j, pl.ds(at, 8), :] for j in range(BASIS)]
                solved = c[0] * u[0]
                left = c[ITERS] * u[0]
                for j in range(1, BASIS):
                    if j < ITERS:
                        solved = solved + c[j] * u[j]
                    left = left + c[ITERS + j] * u[j]
                solution_ref[m, 8 * t : 8 * t + 8] = rolled(solved, -32 * q)
                residual_ref[m, 8 * t : 8 * t + 8] = rolled(diag_ref[q, 8 * t : 8 * t + 8] * left, -32 * q)
        for copy in copies(s):
            copy.start()
        return 0

    def copies(s):
        members = pl.ds(4 * s, 4)
        return [
            pltpu.make_async_copy(source.at[members], target.at[members], sems.at[n, s])
            for n, (source, target) in enumerate(((solution_ref, solved_ref), (residual_ref, left_ref)))
        ]

    lax.fori_loop(0, GROUPS, combine, 0, unroll=2)
    for s in range(GROUPS):
        for copy in copies(s):
            copy.wait()


def shape(*dims):
    return jax.ShapeDtypeStruct(dims, F32)


def call(kernel, inputs, out_shape, scratch=(), name=None, in_specs=None, out_specs=None):
    return pl.pallas_call(
        kernel,
        out_shape=out_shape,
        in_specs=in_specs or [VMEM] * len(inputs),
        out_specs=out_specs or [VMEM] * len(out_shape),
        scratch_shapes=list(scratch),
        interpret=INTERPRET,
        name=name,
        compiler_params=pltpu.CompilerParams(vmem_limit_bytes=28 * 1024 * 1024),
    )(*inputs)


def on_device(right_side, couplings, center, ocean_mask):
    ny, nx = lax.axis_size(GY), lax.axis_size(GX)
    top = (lax.axis_index(GY) == ny - 1).astype(jnp.int32).reshape(1)
    sent = shape(PACKED, LANES)
    right_side, couplings, center, ocean_mask = (
        pltpu.with_memory_space_constraint(a, pltpu.HBM) for a in (right_side, couplings, center, ocean_mask)
    )
    planes, last, first = call(
        edges_kernel, (right_side, couplings, center, ocean_mask), (shape(PLANES, ROWS, LANES), sent, sent),
        scratch=(
            pltpu.VMEM((2, MEMBERS, 8, LANES), F32),
            pltpu.VMEM((ROWS, LANES), F32),
            pltpu.VMEM((ROWS, LANES), jnp.int32),
            pltpu.SemaphoreType.DMA((5,)),
        ),
        name="edges",
        in_specs=[HBM] * 4,
    )
    with jax.named_scope("south"):
        south = lax.ppermute(last, GY, [(k, k + 1) for k in range(ny - 1)])
    with jax.named_scope("north"):
        north = lax.ppermute(first, GY, [(k + 1, k) for k in range(ny - 1)])
    row = (ny - 1) * nx
    turned_last = last[::-1, ::-1]
    with jax.named_scope("fold"):
        fold = lax.ppermute(turned_last, ALL, [(row + k, row + nx - 1 - k) for k in range(nx)])

    inner = shape(3, TILES - 2, 8, LANES)
    turned, inner_west, inner_east = call(
        pack_own_kernel, (right_side, planes), (shape(MEMBERS, ROWS, LANES), inner, inner), name="pack_own",
        scratch=(pltpu.VMEM((MEMBERS, ROWS, LANES), F32), pltpu.SemaphoreType.DMA),
        in_specs=[HBM, VMEM],
    )
    packed = shape(3, TILES, 8, LANES)
    turned_halo, planes_halo, own_west, own_east = call(
        pack_halo_kernel,
        (south, north, fold, inner_west, inner_east),
        (shape(MEMBERS, 2, 8, LANES), shape(PLANES, 2, 8, LANES), packed, packed),
        scratch=(pltpu.VMEM((2, MEMBERS, 8, LANES), F32),),
        name="pack_halo",
    )
    from_west = lax.ppermute(own_east, GX, [(k, (k + 1) % nx) for k in range(nx)])
    from_east = lax.ppermute(own_west, GX, [((k + 1) % nx, k) for k in range(nx)])

    near, far = lax.axis_size(NEAR), lax.axis_size(FAR)
    basis, diag, gram = call(
        basis_kernel,
        (top, turned, turned_halo, planes, planes_halo, own_west, own_east, from_west, from_east),
        (shape(BASIS, 16 + MEMBERS * EXT, LANES), shape(4, ROWS, LANES), shape(near, 8, LANES)),
        scratch=(
            pltpu.VMEM((ITERS, 16 + GROUPS * EXT, LANES), F32),
            pltpu.VMEM((16 + PLANES * EXT, LANES), F32),
            pltpu.VMEM((16 + PLANES * EXT, LANES), F32),
            pltpu.VMEM((TILES, 4, 8, 8, LANES), F32),
            pltpu.VMEM((TILES, 8, 8, LANES), F32),
            pltpu.VMEM((TILES, 4, 8, LANES), F32),
            pltpu.VMEM((TILES, 8, LANES), F32),
            pltpu.VMEM((TILES, GROUPS, 8, LANES), F32),
            pltpu.VMEM((len(PAIRS) * MEMBERS * 8, LANES), F32),
        ),
        name="basis",
        in_specs=[SMEM] + [VMEM] * 8,
    )
    parts = lax.all_to_all(gram, NEAR, 0, 0, tiled=True)
    zero = jnp.zeros((8, LANES), F32)
    mine = jnp.stack(sum2([(parts[k], zero) for k in range(near)]))
    total = lax.all_to_all(jnp.broadcast_to(mine[None], (far, *mine.shape)), FAR, 0, 0, tiled=True)
    return tuple(call(
        finish_kernel,
        (total, basis, diag),
        (shape(MEMBERS, ROWS, LANES), shape(MEMBERS, ROWS, LANES)),
        scratch=(
            pltpu.VMEM((2 * ITERS + 1, MEMBERS, LANES), F32),
            pltpu.VMEM((MEMBERS, ROWS, LANES), F32),
            pltpu.VMEM((MEMBERS, ROWS, LANES), F32),
            pltpu.SemaphoreType.DMA((2, GROUPS)),
        ),
        name="finish",
        out_specs=[HBM, HBM],
    ))


def solution(mesh):
    split = Mesh(mesh.devices.reshape(8, 4, 4, 2), ("gy_0", "gy_1", "gx_0", "gx_1"))
    placed = (P(None, GY, GX), P(None, GY, GX), P(GY, GX), P(GY, GX))
    return jax.shard_map(
        on_device,
        mesh=split,
        in_specs=placed,
        out_specs=(P(None, GY, GX), P(None, GY, GX)),
        check_vma=False,
    )
```

```python
import jax
import jax.numpy as jnp
from jax import lax
from jax.experimental import pallas as pl
from jax.experimental.pallas import tpu as pltpu
from jax.sharding import Mesh
from jax.sharding import PartitionSpec as P


ITERS = 6
SHIFT = (0.375, 0.0, 0.375, 0.0, 0.375, 0.0)
GY = ("gy_0", "gy_1")
GX = ("gx_0", "gx_1")
ALL = GY + GX
NEAR = ("gy_0", "gx_1")
FAR = ("gy_1", "gx_0")
MEMBERS = 32
ROWS = 64
LANES = 128
HALO = 8
TILES = (ROWS + 2 * HALO) // 8
EXT = ROWS + 2 * HALO
GROUPS = MEMBERS // 4
PLANES = 4
BASIS = ITERS + 1
PAIRS = [(i, j) for i in range(ITERS) for j in range(i, BASIS)]
INTERPRET = False
F32 = jnp.float32
VMEM = pl.BlockSpec(memory_space=pltpu.VMEM)
SMEM = pl.BlockSpec(memory_space=pltpu.SMEM)
HBM = pl.BlockSpec(memory_space=pltpu.HBM)


def lanes_of():
    return lax.broadcasted_iota(jnp.int32, (8, LANES), 1)


def rolled(value, shift):
    shift %= LANES
    return value if shift == 0 else pltpu.roll(value, shift, 1)


SENT = 6
PACKED = MEMBERS * SENT + PLANES * 8


def edges_kernel(
    right_ref, couplings_ref, center_ref, mask_ref, planes_ref, last_ref, first_ref, rows_ref, center_row_ref, mask_row_ref, sems
):
    copies = [
        pltpu.make_async_copy(couplings_ref, planes_ref.at[pl.ds(0, 3)], sems.at[0]),
        pltpu.make_async_copy(center_ref, center_row_ref, sems.at[1]),
        pltpu.make_async_copy(mask_ref, mask_row_ref, sems.at[2]),
        pltpu.make_async_copy(right_ref.at[:, pl.ds(ROWS - 8, 8), :], rows_ref.at[0], sems.at[3]),
        pltpu.make_async_copy(right_ref.at[:, pl.ds(0, 8), :], rows_ref.at[1], sems.at[4]),
    ]
    for copy in copies:
        copy.start()
    for copy in copies:
        copy.wait()
    planes_ref[3] = jnp.where(mask_row_ref[...] != 0, center_row_ref[...], 0.0)
    for p in range(PLANES):
        base = MEMBERS * SENT + 8 * p
        last_ref[base : base + 8] = planes_ref[p, ROWS - 8 : ROWS]
        first_ref[base : base + 8] = planes_ref[p, 0:8]
    for m in range(MEMBERS):
        last_ref[SENT * m : SENT * m + SENT] = rows_ref[0, m, 8 - SENT : 8]
        first_ref[SENT * m : SENT * m + SENT] = rows_ref[1, m, 0:SENT]


def pack(load, store, west_ref, east_ref, tile):
    window = lanes_of() // 8
    for h in range(3):
        members = range(16 * h, 16 * h + 16) if h < 2 else range(MEMBERS, MEMBERS + PLANES)
        first = last = None
        for m in members:
            value = rolled(load(m), 32 * (m % 4))
            if m < MEMBERS:
                store(m, value)
            extra = 8 * (m // 4 % 4) if h < 2 else 0
            low, high = rolled(value, extra), rolled(value, extra + 8)
            if first is None:
                first, last = low, high
            else:
                here = window == 4 * (m % 4) + extra // 8
                first = jnp.where(here, low, first)
                last = jnp.where(here, high, last)
        west_ref[h, tile] = first
        east_ref[h, tile] = last


def pack_own_kernel(right_hbm_ref, planes_ref, turned_ref, west_ref, east_ref, right_ref, sem):
    copy = pltpu.make_async_copy(right_hbm_ref, right_ref, sem)
    copy.start()
    copy.wait()

    def own(t, _):
        at = pl.multiple_of(8 * t, 8)

        def load(m):
            return right_ref[m, pl.ds(at, 8), :] if m < MEMBERS else planes_ref[m - MEMBERS, pl.ds(at, 8), :]

        def store(m, value):
            turned_ref[m, pl.ds(at, 8), :] = value

        pack(load, store, west_ref, east_ref, t)
        return 0

    lax.fori_loop(0, ROWS // 8, own, 0)


def pack_halo_kernel(
    south_ref, north_ref, fold_ref, own_west_ref, own_east_ref, turned_ref, planes_ref, west_ref, east_ref, rows_ref
):
    for h in range(3):
        west_ref[h, 1 : TILES - 1] = own_west_ref[h]
        east_ref[h, 1 : TILES - 1] = own_east_ref[h]
    zero = jnp.zeros((8, LANES), F32)
    for m in range(MEMBERS):
        rows_ref[0, m] = zero
        rows_ref[1, m] = zero
        rows_ref[0, m, 8 - SENT : 8] = south_ref[SENT * m : SENT * m + SENT]
        back = PACKED - SENT * (m + 1)
        rows_ref[1, m, 0:SENT] = north_ref[SENT * m : SENT * m + SENT] + fold_ref[back : back + SENT]
    for p in range(PLANES):
        base = MEMBERS * SENT + 8 * p
        back = PACKED - base - 8
        planes_ref[p, 0] = south_ref[base : base + 8]
        planes_ref[p, 1] = north_ref[base : base + 8] + fold_ref[back : back + 8]
    for k, tile in ((0, 0), (1, TILES - 1)):
        def load(m, k=k):
            return rows_ref[k, m] if m < MEMBERS else planes_ref[m - MEMBERS, k]

        def store(m, value, k=k):
            turned_ref[m, k] = value

        pack(load, store, west_ref, east_ref, tile)


def basis_kernel(
    top_ref, right_ref, right_halo_ref, planes_ref, planes_halo_ref,
    own_west_ref, own_east_ref, from_west_ref, from_east_ref,
    basis_ref, diag_ref, gram_ref,
    strip_ref, plane_ref, plane_strip_ref, weight_ref, weight_strip_ref, inverse_ref, inverse_strip_ref,
    edge_ref, partial_ref,
):
    lane = lanes_of()
    spot = (lane + 7) % 32

    def main_row(member, tile):
        return 8 + member * EXT + 8 * tile

    def at8(row):
        return pl.ds(pl.multiple_of(row, 8), 8)

    zero = jnp.zeros((8, LANES), F32)
    for j in range(ITERS):
        basis_ref[j, 0:8] = zero
        basis_ref[j, 8 + MEMBERS * EXT : 16 + MEMBERS * EXT] = zero
        strip_ref[j, 0:8] = zero
        strip_ref[j, 8 + GROUPS * EXT : 16 + GROUPS * EXT] = zero

    for p in range(PLANES):
        base = 8 + p * EXT
        plane_ref[base : base + 8] = planes_halo_ref[p, 0]
        plane_ref[base + 8 : base + 8 + ROWS] = planes_ref[p]
        plane_ref[base + 8 + ROWS : base + EXT] = planes_halo_ref[p, 1]
    plane_ref[0:8] = zero
    plane_ref[8 + PLANES * EXT : 16 + PLANES * EXT] = zero
    plane_strip_ref[0:8] = zero
    plane_strip_ref[8 + PLANES * EXT : 16 + PLANES * EXT] = zero

    def joined(h, tile, at):
        out = rolled(from_west_ref[h, tile], -7 - at)
        out = jnp.where(spot < 8, out, rolled(own_west_ref[h, tile], 1 - at))
        out = jnp.where(spot < 16, out, rolled(own_east_ref[h, tile], 9 - at))
        return jnp.where(spot < 24, out, rolled(from_east_ref[h, tile], 17 - at))

    def plane_strips(t, _):
        value = joined(2, t, 0)
        for p in range(PLANES):
            one = jnp.where((lane + 7) // 32 % 4 == p, value, 0.0)
            one = one + pltpu.roll(one, 32, 1)
            one = one + pltpu.roll(one, 64, 1)
            plane_strip_ref[at8(8 + p * EXT + 8 * t), :] = one
        return 0

    lax.fori_loop(0, TILES, plane_strips, 0, unroll=True)

    def weights(t, ghost):
        dr = 1 if ghost else -1
        side = LANES - 1 if ghost else 1

        def row(ref, p, shift):
            return ref[pl.ds(8 + p * EXT + 8 * t + shift, 8), :]

        def beside(main, strip):
            if ghost:
                return jnp.where(lane == LANES - 1, pltpu.roll(strip, 110, 1), pltpu.roll(main, side, 1))
            return jnp.where(lane == 0, strip, pltpu.roll(main, side, 1))

        def finish(cn0, cnr, ce0, cec, cc0, ccr, ccc, ccrc, center, main):
            total = center + cn0 + cnr + ce0 + cec + cc0 + ccr + ccc + ccrc
            inv = jnp.where(center > 0.0, 1.0 / total, 0.0)
            if ghost:
                w = dict(s=cn0, n=cnr, w=ce0, e=cec, sw=cc0, nw=ccr, se=ccc, ne=ccrc)
            else:
                w = dict(n=cn0, s=cnr, e=ce0, w=cec, ne=cc0, se=ccr, nw=ccc, sw=ccrc)

            def ahead(value):
                value = pltpu.roll(value * inv, 1, 1)
                return jnp.where(lane == 0, 0.0, value) if main else value

            def behind(value):
                value = pltpu.roll(value * inv, LANES - 1, 1)
                return jnp.where(lane == LANES - 1, 0.0, value) if main else value

            return total, inv, (
                w["s"] * inv, w["n"] * inv,
                ahead(w["se"]), ahead(w["e"]), ahead(w["ne"]),
                behind(w["sw"]), behind(w["w"]), behind(w["nw"]),
            )

        strips = [row(plane_strip_ref, p, 0) for p in range(PLANES)]
        strips_r = [row(plane_strip_ref, p, dr) for p in (0, 2)]
        _, inv, ws = finish(
            strips[0], strips_r[0], strips[1], pltpu.roll(strips[1], side, 1),
            strips[2], strips_r[1], pltpu.roll(strips[2], side, 1), pltpu.roll(strips_r[1], side, 1),
            strips[3], False,
        )
        inverse_strip_ref[t] = inv
        for k in range(8):
            weight_strip_ref[t, k] = ws[k]
        mains = [row(plane_ref, p, 0) for p in range(PLANES)]
        mains_r = [row(plane_ref, p, dr) for p in (0, 2)]
        total, inv, ws = finish(
            mains[0], mains_r[0], mains[1], beside(mains[1], strips[1]),
            mains[2], mains_r[1], beside(mains[2], strips[2]), beside(mains_r[1], strips_r[1]),
            mains[3], True,
        )
        for q in range(4):
            inverse_ref[t, q] = rolled(inv, 32 * q)
            for k in range(8):
                weight_ref[t, q, k] = rolled(ws[k], 32 * q)
        return total

    weights(0, False)

    def inner_weights(t, _):
        total = weights(t, False)
        for q in range(4):
            diag_ref[q, at8(8 * (t - 1)), :] = rolled(total, 32 * q)
        return 0

    lax.fori_loop(1, TILES - 1, inner_weights, 0, unroll=True)

    @pl.when(top_ref[0] == 0)
    def _():
        weights(TILES - 1, False)

    @pl.when(top_ref[0] != 0)
    def _():
        weights(TILES - 1, True)

    def first(t, load):
        for q in range(4):
            inv = inverse_ref[t, q]
            for s in range(GROUPS):
                m = 4 * s + q
                basis_ref[0, at8(main_row(m, t)), :] = load(m) * inv
        inv = inverse_strip_ref[t]
        for s in range(GROUPS):
            strip_ref[0, at8(8 + s * EXT + 8 * t), :] = joined(s // 4, t, 8 * (s % 4)) * inv

    first(0, lambda m: right_halo_ref[m, 0])

    def inner_first(t, _):
        first(t, lambda m: right_ref[m, at8(8 * (t - 1)), :])
        return 0

    lax.fori_loop(1, TILES - 1, inner_first, 0, unroll=True)
    first(TILES - 1, lambda m: right_halo_ref[m, 1])

    def parts(ref, j, base, w):
        a = ref[j, pl.ds(base - 1, 8), :]
        b = ref[j, at8(base), :]
        c = ref[j, pl.ds(base + 1, 8), :]
        middle = w[0] * a + w[1] * c
        if SHIFT[j]:
            middle = middle - SHIFT[j] * b
        return middle, (w[2] * a + w[4] * c) + w[3] * b, (w[5] * a + w[7] * c) + w[6] * b

    def staged(work):
        begun = [(end, begin()) for begin, end in work]
        for end, values in begun:
            end(values)

    def strip_work(j, t):
        def begin():
            w = [weight_strip_ref[t, k] for k in range(8)]
            values = []
            for s in range(GROUPS):
                middle, ahead, behind = parts(strip_ref, j, 8 + s * EXT + 8 * t, w)
                edge = jnp.where(lane % 32 == 31, pltpu.roll(ahead, LANES - 18, 1), behind)
                moved = (pltpu.roll(ahead, LANES - 1, 1), pltpu.roll(behind, 1, 1)) if j + 1 < ITERS else ()
                values.append((middle, edge, moved))
            return values

        def end(values):
            for s, (middle, edge, moved) in enumerate(values):
                edge_ref[j % 2, t, s] = edge
                if moved:
                    strip_ref[j + 1, at8(8 + s * EXT + 8 * t), :] = middle + moved[0] + moved[1]

        return begin, end

    def main_work(j, t, q, groups):
        def begin():
            w = [weight_ref[t, q, k] for k in range(8)]
            ends = (lane == 32 * q) | (lane == (32 * q - 1) % LANES)
            values = []
            for s in groups:
                middle, ahead, behind = parts(basis_ref, j, main_row(4 * s + q, t), w)
                middle = middle + jnp.where(ends, edge_ref[j % 2, t, s], 0.0)
                values.append((middle, pltpu.roll(ahead, LANES - 1, 1), pltpu.roll(behind, 1, 1)))
            return values

        def end(values):
            for s, (middle, ahead, behind) in zip(groups, values):
                basis_ref[j + 1, at8(main_row(4 * s + q, t)), :] = middle + ahead + behind

        return begin, end

    def span(j, n):
        low, high = (0, TILES) if j + 1 < ITERS else (1, TILES - 1)
        half = (high - low) // 2
        return [low + half * n + k for k in range(half)]

    staged([strip_work(0, t) for n in range(2) for t in span(0, n)])
    for j in range(ITERS):
        def body(n, _, j=j):
            work = [main_work(j, t, q, range(GROUPS)) for t in span(j, n) for q in range(4)]
            if j + 1 < ITERS:
                work += [strip_work(j + 1, t) for t in span(j + 1, n)]
            staged(work)
            return 0

        lax.fori_loop(0, 2, body, 0)

    def products(s, _):
        for q in range(4):
            m = 4 * s + q
            sums = [None] * len(PAIRS)
            for t in range(1, TILES - 1):
                u = [basis_ref[j, at8(main_row(m, t)), :] for j in range(BASIS)]
                d = diag_ref[q, 8 * (t - 1) : 8 * t]
                scaled = [d * u[j] for j in range(ITERS)]
                for n, (i, j) in enumerate(PAIRS):
                    term = scaled[i] * u[j]
                    sums[n] = term if sums[n] is None else sums[n] + term
            for n in range(len(PAIRS)):
                partial_ref[at8((n * MEMBERS + m) * 8), :] = sums[n]
        return 0

    lax.fori_loop(0, GROUPS, products, 0)
    result = zero
    for l in range(len(PAIRS) * MEMBERS // 8):
        rows = [partial_ref[pl.ds(64 * l + k, 8, stride=8), :] for k in range(8)]
        while len(rows) > 1:
            rows = [rows[k] + rows[k + 1] for k in range(0, len(rows), 2)]
        result = jnp.where(lane == l, jnp.sum(rows[0], axis=1, keepdims=True), result)
    for n in range(gram_ref.shape[0]):
        gram_ref[n] = result


def two_sum(a, b):
    s = a + b
    t = s - a
    return s, (a - (s - t)) + (b - t)


def quick(a, b):
    s = a + b
    return s, b - (s - a)


def halves(a):
    t = 4097.0 * a
    high = t - (t - a)
    return high, a - high


def add2(a, b):
    s, e = two_sum(a[0], b[0])
    return quick(s, e + (a[1] + b[1]))


def mul2(a, b):
    p = a[0] * b[0]
    ah, al = halves(a[0])
    bh, bl = halves(b[0])
    e = ((ah * bh - p) + ah * bl + al * bh) + al * bl
    return quick(p, e + (a[0] * b[1] + a[1] * b[0]))


def neg2(a):
    return -a[0], -a[1]


def div2(a, b):
    q = a[0] / b[0]
    zero = jnp.zeros_like(q)
    rest = add2(a, neg2(mul2((q, zero), b)))
    return quick(q, rest[0] / b[0])


def sum2(terms):
    terms = list(terms)
    while len(terms) > 1:
        terms = [add2(terms[k], terms[k + 1]) if k + 1 < len(terms) else terms[k] for k in range(0, len(terms), 2)]
    return terms[0]


def finish_kernel(total_ref, basis_ref, diag_ref, solved_ref, left_ref, coeff_ref, solution_ref, residual_ref, sems):
    count = total_ref.shape[0]
    high, low = sum2([(total_ref[n, 0], total_ref[n, 1]) for n in range(count)])
    gram = {}
    for n, (i, j) in enumerate(PAIRS):
        shift = (LANES - 4 * n) % LANES
        value = (high, low) if shift == 0 else (pltpu.roll(high, shift, 1), pltpu.roll(low, shift, 1))
        gram[i, j] = gram[j, i] = value

    def scaled(value, factor):
        if factor == 1.0:
            return value
        s, e = two_sum(0.5 * value[0], 0.125 * value[0])
        return quick(s, e + factor * value[1])

    def dot(a, b):
        return sum2([mul2(x, y) for x, y in zip(a, b)])

    one = (jnp.ones((8, LANES), F32), jnp.zeros((8, LANES), F32))
    precond, direction, answer = [one], [one], []
    rz = gram[0, 0]
    for k in range(ITERS):
        image = [scaled(c, 1.0 - SHIFT[j]) for j, c in enumerate(direction)]
        image = [image[0]] + [
            add2(image[j], neg2(direction[j - 1])) for j in range(1, k + 1)
        ] + [neg2(direction[k])]
        final = k + 1 == ITERS
        row = [dot([gram[i, j] for j in range(k + 2)], image) for i in range(k + 1 if final else k + 2)]
        step_size = div2(rz, dot(direction, row))
        moved = [mul2(step_size, c) for c in direction]
        answer = [add2(a, b) for a, b in zip(answer, moved)] + moved[len(answer):]
        if not final:
            cross = dot(precond, row)
            rz_new = mul2(step_size, add2(mul2(step_size, dot(image, row)), (-2.0 * cross[0], -2.0 * cross[1])))
            rz_new = add2(rz, rz_new)
        moved = [neg2(mul2(step_size, c)) for c in image]
        precond = [add2(a, b) for a, b in zip(precond, moved)] + moved[len(precond):]
        if not final:
            ratio = div2(rz_new, rz)
            moved = [mul2(ratio, c) for c in direction]
            direction = [add2(a, b) for a, b in zip(precond, moved)] + precond[len(moved):]
            rz = rz_new

    values = [c[0] for c in answer] + [c[0] for c in precond]
    for n, value in enumerate(values):
        for l in range(MEMBERS // 8):
            coeff_ref[n, 8 * l : 8 * l + 8] = jnp.broadcast_to(value[:, l : l + 1], (8, LANES))

    def combine(s, _):
        for q in range(4):
            m = 4 * s + q
            c = [jnp.broadcast_to(coeff_ref[n, pl.ds(m, 1), :], (8, LANES)) for n in range(2 * ITERS + 1)]
            for t in range(ROWS // 8):
                at = pl.multiple_of(16 + m * EXT + 8 * t, 8)
                u = [basis_ref[j, pl.ds(at, 8), :] for j in range(BASIS)]
                solved = c[0] * u[0]
                left = c[ITERS] * u[0]
                for j in range(1, BASIS):
                    if j < ITERS:
                        solved = solved + c[j] * u[j]
                    left = left + c[ITERS + j] * u[j]
                solution_ref[m, 8 * t : 8 * t + 8] = rolled(solved, -32 * q)
                residual_ref[m, 8 * t : 8 * t + 8] = rolled(diag_ref[q, 8 * t : 8 * t + 8] * left, -32 * q)
        for copy in copies(s):
            copy.start()
        return 0

    def copies(s):
        members = pl.ds(4 * s, 4)
        return [
            pltpu.make_async_copy(source.at[members], target.at[members], sems.at[n, s])
            for n, (source, target) in enumerate(((solution_ref, solved_ref), (residual_ref, left_ref)))
        ]

    lax.fori_loop(0, GROUPS, combine, 0, unroll=2)
    for s in range(GROUPS):
        for copy in copies(s):
            copy.wait()


def shape(*dims):
    return jax.ShapeDtypeStruct(dims, F32)


def call(kernel, inputs, out_shape, scratch=(), in_specs=None, out_specs=None):
    return pl.pallas_call(
        kernel,
        out_shape=out_shape,
        in_specs=in_specs or [VMEM] * len(inputs),
        out_specs=out_specs or [VMEM] * len(out_shape),
        scratch_shapes=list(scratch),
        interpret=INTERPRET,
        compiler_params=pltpu.CompilerParams(vmem_limit_bytes=28 * 1024 * 1024),
    )(*inputs)


def on_device(right_side, couplings, center, ocean_mask):
    ny, nx = lax.axis_size(GY), lax.axis_size(GX)
    top = (lax.axis_index(GY) == ny - 1).astype(jnp.int32).reshape(1)
    sent = shape(PACKED, LANES)
    right_side, couplings, center, ocean_mask = (
        pltpu.with_memory_space_constraint(a, pltpu.HBM) for a in (right_side, couplings, center, ocean_mask)
    )
    planes, last, first = call(
        edges_kernel, (right_side, couplings, center, ocean_mask), (shape(PLANES, ROWS, LANES), sent, sent),
        scratch=(
            pltpu.VMEM((2, MEMBERS, 8, LANES), F32),
            pltpu.VMEM((ROWS, LANES), F32),
            pltpu.VMEM((ROWS, LANES), jnp.int32),
            pltpu.SemaphoreType.DMA((5,)),
        ),
        in_specs=[HBM] * 4,
    )
    south = lax.ppermute(last, GY, [(k, k + 1) for k in range(ny - 1)])
    north = lax.ppermute(first, GY, [(k + 1, k) for k in range(ny - 1)])
    row = (ny - 1) * nx
    turned_last = last[::-1, ::-1]
    fold = lax.ppermute(turned_last, ALL, [(row + k, row + nx - 1 - k) for k in range(nx)])

    inner = shape(3, TILES - 2, 8, LANES)
    turned, inner_west, inner_east = call(
        pack_own_kernel, (right_side, planes), (shape(MEMBERS, ROWS, LANES), inner, inner),
        scratch=(pltpu.VMEM((MEMBERS, ROWS, LANES), F32), pltpu.SemaphoreType.DMA),
        in_specs=[HBM, VMEM],
    )
    packed = shape(3, TILES, 8, LANES)
    turned_halo, planes_halo, own_west, own_east = call(
        pack_halo_kernel,
        (south, north, fold, inner_west, inner_east),
        (shape(MEMBERS, 2, 8, LANES), shape(PLANES, 2, 8, LANES), packed, packed),
        scratch=(pltpu.VMEM((2, MEMBERS, 8, LANES), F32),),
    )
    from_west = lax.ppermute(own_east, GX, [(k, (k + 1) % nx) for k in range(nx)])
    from_east = lax.ppermute(own_west, GX, [((k + 1) % nx, k) for k in range(nx)])

    near, far = lax.axis_size(NEAR), lax.axis_size(FAR)
    basis, diag, gram = call(
        basis_kernel,
        (top, turned, turned_halo, planes, planes_halo, own_west, own_east, from_west, from_east),
        (shape(BASIS, 16 + MEMBERS * EXT, LANES), shape(4, ROWS, LANES), shape(near, 8, LANES)),
        scratch=(
            pltpu.VMEM((ITERS, 16 + GROUPS * EXT, LANES), F32),
            pltpu.VMEM((16 + PLANES * EXT, LANES), F32),
            pltpu.VMEM((16 + PLANES * EXT, LANES), F32),
            pltpu.VMEM((TILES, 4, 8, 8, LANES), F32),
            pltpu.VMEM((TILES, 8, 8, LANES), F32),
            pltpu.VMEM((TILES, 4, 8, LANES), F32),
            pltpu.VMEM((TILES, 8, LANES), F32),
            pltpu.VMEM((2, TILES, GROUPS, 8, LANES), F32),
            pltpu.VMEM((len(PAIRS) * MEMBERS * 8, LANES), F32),
        ),
        in_specs=[SMEM] + [VMEM] * 8,
    )
    parts = lax.all_to_all(gram, NEAR, 0, 0, tiled=True)
    zero = jnp.zeros((8, LANES), F32)
    mine = jnp.stack(sum2([(parts[k], zero) for k in range(near)]))
    total = lax.all_to_all(jnp.broadcast_to(mine[None], (far, *mine.shape)), FAR, 0, 0, tiled=True)
    return tuple(call(
        finish_kernel,
        (total, basis, diag),
        (shape(MEMBERS, ROWS, LANES), shape(MEMBERS, ROWS, LANES)),
        scratch=(
            pltpu.VMEM((2 * ITERS + 1, MEMBERS, LANES), F32),
            pltpu.VMEM((MEMBERS, ROWS, LANES), F32),
            pltpu.VMEM((MEMBERS, ROWS, LANES), F32),
            pltpu.SemaphoreType.DMA((2, GROUPS)),
        ),
        out_specs=[HBM, HBM],
    ))


def solution(mesh):
    split = Mesh(mesh.devices.reshape(8, 4, 4, 2), ("gy_0", "gy_1", "gx_0", "gx_1"))
    placed = (P(None, GY, GX), P(None, GY, GX), P(GY, GX), P(GY, GX))
    return jax.shard_map(
        on_device,
        mesh=split,
        in_specs=placed,
        out_specs=(P(None, GY, GX), P(None, GY, GX)),
        check_vma=False,
    )
```

```python
import jax
import jax.numpy as jnp
from jax import lax
from jax.experimental import pallas as pl
from jax.experimental.pallas import tpu as pltpu
from jax.sharding import Mesh
from jax.sharding import PartitionSpec as P


ITERS = 6
SHIFT = (0.375, 0.0, 0.375, 0.0, 0.375, 0.0)
GY = ("gy_0", "gy_1")
GX = ("gx_0", "gx_1")
ALL = GY + GX
NEAR = ("gy_0", "gx_1")
FAR = ("gy_1", "gx_0")
MEMBERS = 32
ROWS = 64
LANES = 128
HALO = 8
TILES = (ROWS + 2 * HALO) // 8
EXT = ROWS + 2 * HALO
GROUPS = MEMBERS // 4
PLANES = 4
BASIS = ITERS + 1
PAIRS = [(i, j) for i in range(ITERS) for j in range(i, BASIS)]
INTERPRET = False
F32 = jnp.float32
VMEM = pl.BlockSpec(memory_space=pltpu.VMEM)
SMEM = pl.BlockSpec(memory_space=pltpu.SMEM)
HBM = pl.BlockSpec(memory_space=pltpu.HBM)


def lanes_of():
    return lax.broadcasted_iota(jnp.int32, (8, LANES), 1)


def rolled(value, shift):
    shift %= LANES
    return value if shift == 0 else pltpu.roll(value, shift, 1)


SENT = 6
PACKED = MEMBERS * SENT + PLANES * 8


def edges_kernel(
    right_ref, couplings_ref, center_ref, mask_ref, planes_ref, last_ref, first_ref, rows_ref, center_row_ref, mask_row_ref, sems
):
    copies = [
        pltpu.make_async_copy(couplings_ref, planes_ref.at[pl.ds(0, 3)], sems.at[0]),
        pltpu.make_async_copy(center_ref, center_row_ref, sems.at[1]),
        pltpu.make_async_copy(mask_ref, mask_row_ref, sems.at[2]),
        pltpu.make_async_copy(right_ref.at[:, pl.ds(ROWS - 8, 8), :], rows_ref.at[0], sems.at[3]),
        pltpu.make_async_copy(right_ref.at[:, pl.ds(0, 8), :], rows_ref.at[1], sems.at[4]),
    ]
    for copy in copies:
        copy.start()
    for copy in copies:
        copy.wait()
    planes_ref[3] = jnp.where(mask_row_ref[...] != 0, center_row_ref[...], 0.0)
    for p in range(PLANES):
        base = MEMBERS * SENT + 8 * p
        last_ref[base : base + 8] = planes_ref[p, ROWS - 8 : ROWS]
        first_ref[base : base + 8] = planes_ref[p, 0:8]
    for m in range(MEMBERS):
        last_ref[SENT * m : SENT * m + SENT] = rows_ref[0, m, 8 - SENT : 8]
        first_ref[SENT * m : SENT * m + SENT] = rows_ref[1, m, 0:SENT]


def pack(load, store, west_ref, east_ref, tile):
    window = lanes_of() // 8
    for h in range(3):
        members = range(16 * h, 16 * h + 16) if h < 2 else range(MEMBERS, MEMBERS + PLANES)
        first = last = None
        for m in members:
            value = rolled(load(m), 32 * (m % 4))
            if m < MEMBERS:
                store(m, value)
            extra = 8 * (m // 4 % 4) if h < 2 else 0
            low, high = rolled(value, extra), rolled(value, extra + 8)
            if first is None:
                first, last = low, high
            else:
                here = window == 4 * (m % 4) + extra // 8
                first = jnp.where(here, low, first)
                last = jnp.where(here, high, last)
        west_ref[h, tile] = first
        east_ref[h, tile] = last


def pack_own_kernel(right_hbm_ref, planes_ref, turned_ref, west_ref, east_ref, right_ref, sem):
    copy = pltpu.make_async_copy(right_hbm_ref, right_ref, sem)
    copy.start()
    copy.wait()

    def own(t, _):
        at = pl.multiple_of(8 * t, 8)

        def load(m):
            return right_ref[m, pl.ds(at, 8), :] if m < MEMBERS else planes_ref[m - MEMBERS, pl.ds(at, 8), :]

        def store(m, value):
            turned_ref[m, pl.ds(at, 8), :] = value

        pack(load, store, west_ref, east_ref, t)
        return 0

    lax.fori_loop(0, ROWS // 8, own, 0)


def pack_halo_kernel(
    south_ref, north_ref, fold_ref, own_west_ref, own_east_ref, turned_ref, planes_ref, west_ref, east_ref, rows_ref,
    ends_west_ref, ends_east_ref,
):
    for h in range(2):
        west_ref[TILES * h + 1 : TILES * (h + 1) - 1] = own_west_ref[h]
        east_ref[TILES * h + 1 : TILES * (h + 1) - 1] = own_east_ref[h]
    zero = jnp.zeros((8, LANES), F32)
    for m in range(MEMBERS):
        rows_ref[0, m] = zero
        rows_ref[1, m] = zero
        rows_ref[0, m, 8 - SENT : 8] = south_ref[SENT * m : SENT * m + SENT]
        back = PACKED - SENT * (m + 1)
        rows_ref[1, m, 0:SENT] = north_ref[SENT * m : SENT * m + SENT] + fold_ref[back : back + SENT]
    for p in range(PLANES):
        base = MEMBERS * SENT + 8 * p
        back = PACKED - base - 8
        planes_ref[p, 0] = south_ref[base : base + 8]
        planes_ref[p, 1] = north_ref[base : base + 8] + fold_ref[back : back + 8]
    for k, tile in ((0, 0), (1, TILES - 1)):
        def load(m, k=k):
            return rows_ref[k, m] if m < MEMBERS else planes_ref[m - MEMBERS, k]

        def store(m, value, k=k):
            turned_ref[m, k] = value

        pack(load, store, ends_west_ref, ends_east_ref, k)
        for h in range(2):
            west_ref[TILES * h + tile] = ends_west_ref[h, k]
            east_ref[TILES * h + tile] = ends_east_ref[h, k]
    part = lanes_of() % 32 // 8
    for out_ref, own_ref, ends_ref in ((west_ref, own_west_ref, ends_west_ref), (east_ref, own_east_ref, ends_east_ref)):
        for n in range((TILES + 3) // 4):
            value = None
            for tile in range(4 * n, min(4 * n + 4, TILES)):
                one = ends_ref[2, 0] if tile == 0 else ends_ref[2, 1] if tile == TILES - 1 else own_ref[2, tile - 1]
                one = rolled(one, 8 * (tile % 4))
                value = one if value is None else jnp.where(part == tile % 4, one, value)
            out_ref[2 * TILES + n] = value


def basis_kernel(
    top_ref, right_ref, right_halo_ref, planes_ref, planes_halo_ref,
    own_west_ref, own_east_ref, from_west_ref, from_east_ref,
    basis_ref, diag_ref, gram_ref,
    strip_ref, plane_ref, plane_strip_ref, weight_ref, weight_strip_ref, inverse_ref, inverse_strip_ref,
    edge_ref, partial_ref,
):
    lane = lanes_of()
    spot = (lane + 7) % 32

    def main_row(member, tile):
        return 8 + member * EXT + 8 * tile

    def at8(row):
        return pl.ds(pl.multiple_of(row, 8), 8)

    zero = jnp.zeros((8, LANES), F32)
    for j in range(ITERS):
        basis_ref[j, 0:8] = zero
        basis_ref[j, 8 + MEMBERS * EXT : 16 + MEMBERS * EXT] = zero
        strip_ref[j, 0:8] = zero
        strip_ref[j, 8 + GROUPS * EXT : 16 + GROUPS * EXT] = zero

    for p in range(PLANES):
        base = 8 + p * EXT
        plane_ref[base : base + 8] = planes_halo_ref[p, 0]
        plane_ref[base + 8 : base + 8 + ROWS] = planes_ref[p]
        plane_ref[base + 8 + ROWS : base + EXT] = planes_halo_ref[p, 1]
    plane_ref[0:8] = zero
    plane_ref[8 + PLANES * EXT : 16 + PLANES * EXT] = zero
    plane_strip_ref[0:8] = zero
    plane_strip_ref[8 + PLANES * EXT : 16 + PLANES * EXT] = zero

    def joined(n, at):
        out = rolled(from_west_ref[n], -7 - at)
        out = jnp.where(spot < 8, out, rolled(own_west_ref[n], 1 - at))
        out = jnp.where(spot < 16, out, rolled(own_east_ref[n], 9 - at))
        return jnp.where(spot < 24, out, rolled(from_east_ref[n], 17 - at))

    for t in range(TILES):
        value = joined(2 * TILES + t // 4, 8 * (t % 4))
        for p in range(PLANES):
            one = jnp.where((lane + 7) // 32 % 4 == p, value, 0.0)
            one = one + pltpu.roll(one, 32, 1)
            one = one + pltpu.roll(one, 64, 1)
            plane_strip_ref[8 + p * EXT + 8 * t : 16 + p * EXT + 8 * t] = one

    def weights(t, ghost):
        dr = 1 if ghost else -1
        side = LANES - 1 if ghost else 1

        def row(ref, p, shift):
            return ref[pl.ds(8 + p * EXT + 8 * t + shift, 8), :]

        def beside(main, strip):
            if ghost:
                return jnp.where(lane == LANES - 1, pltpu.roll(strip, 110, 1), pltpu.roll(main, side, 1))
            return jnp.where(lane == 0, strip, pltpu.roll(main, side, 1))

        def finish(cn0, cnr, ce0, cec, cc0, ccr, ccc, ccrc, center, main):
            total = center + cn0 + cnr + ce0 + cec + cc0 + ccr + ccc + ccrc
            inv = jnp.where(center > 0.0, 1.0 / total, 0.0)
            if ghost:
                w = dict(s=cn0, n=cnr, w=ce0, e=cec, sw=cc0, nw=ccr, se=ccc, ne=ccrc)
            else:
                w = dict(n=cn0, s=cnr, e=ce0, w=cec, ne=cc0, se=ccr, nw=ccc, sw=ccrc)

            def ahead(value):
                value = pltpu.roll(value * inv, 1, 1)
                return jnp.where(lane == 0, 0.0, value) if main else value

            def behind(value):
                value = pltpu.roll(value * inv, LANES - 1, 1)
                return jnp.where(lane == LANES - 1, 0.0, value) if main else value

            return total, inv, (
                w["s"] * inv, w["n"] * inv,
                ahead(w["se"]), ahead(w["e"]), ahead(w["ne"]),
                behind(w["sw"]), behind(w["w"]), behind(w["nw"]),
            )

        strips = [row(plane_strip_ref, p, 0) for p in range(PLANES)]
        strips_r = [row(plane_strip_ref, p, dr) for p in (0, 2)]
        _, inv, ws = finish(
            strips[0], strips_r[0], strips[1], pltpu.roll(strips[1], side, 1),
            strips[2], strips_r[1], pltpu.roll(strips[2], side, 1), pltpu.roll(strips_r[1], side, 1),
            strips[3], False,
        )
        inverse_strip_ref[t] = inv
        for k in range(8):
            weight_strip_ref[t, k] = ws[k]
        mains = [row(plane_ref, p, 0) for p in range(PLANES)]
        mains_r = [row(plane_ref, p, dr) for p in (0, 2)]
        total, inv, ws = finish(
            mains[0], mains_r[0], mains[1], beside(mains[1], strips[1]),
            mains[2], mains_r[1], beside(mains[2], strips[2]), beside(mains_r[1], strips_r[1]),
            mains[3], True,
        )
        for q in range(4):
            inverse_ref[t, q] = rolled(inv, 32 * q)
            for k in range(8):
                weight_ref[t, q, k] = rolled(ws[k], 32 * q)
        return total

    weights(0, False)

    def inner_weights(t, _):
        total = weights(t, False)
        for q in range(4):
            diag_ref[q, at8(8 * (t - 1)), :] = rolled(total, 32 * q)
        return 0

    lax.fori_loop(1, TILES - 1, inner_weights, 0, unroll=True)

    @pl.when(top_ref[0] == 0)
    def _():
        weights(TILES - 1, False)

    @pl.when(top_ref[0] != 0)
    def _():
        weights(TILES - 1, True)

    def first(t, load):
        for q in range(4):
            inv = inverse_ref[t, q]
            for s in range(GROUPS):
                m = 4 * s + q
                basis_ref[0, at8(main_row(m, t)), :] = load(m) * inv
        inv = inverse_strip_ref[t]
        for s in range(GROUPS):
            strip_ref[0, at8(8 + s * EXT + 8 * t), :] = joined(TILES * (s // 4) + t, 8 * (s % 4)) * inv

    first(0, lambda m: right_halo_ref[m, 0])

    def inner_first(t, _):
        first(t, lambda m: right_ref[m, at8(8 * (t - 1)), :])
        return 0

    lax.fori_loop(1, TILES - 1, inner_first, 0, unroll=True)
    first(TILES - 1, lambda m: right_halo_ref[m, 1])

    def parts(ref, j, base, w):
        a = ref[j, pl.ds(base - 1, 8), :]
        b = ref[j, at8(base), :]
        c = ref[j, pl.ds(base + 1, 8), :]
        middle = w[0] * a + w[1] * c
        if SHIFT[j]:
            middle = middle - SHIFT[j] * b
        return middle, (w[2] * a + w[4] * c) + w[3] * b, (w[5] * a + w[7] * c) + w[6] * b

    def staged(work):
        begun = [(end, begin()) for begin, end in work]
        for end, values in begun:
            end(values)

    def strip_work(j, t):
        def begin():
            w = [weight_strip_ref[t, k] for k in range(8)]
            values = []
            for s in range(GROUPS):
                middle, ahead, behind = parts(strip_ref, j, 8 + s * EXT + 8 * t, w)
                edge = jnp.where(lane % 32 == 31, pltpu.roll(ahead, LANES - 18, 1), behind)
                moved = (pltpu.roll(ahead, LANES - 1, 1), pltpu.roll(behind, 1, 1)) if j + 1 < ITERS else ()
                values.append((middle, edge, moved))
            return values

        def end(values):
            for s, (middle, edge, moved) in enumerate(values):
                edge_ref[j % 2, t, s] = edge
                if moved:
                    strip_ref[j + 1, at8(8 + s * EXT + 8 * t), :] = middle + moved[0] + moved[1]

        return begin, end

    def main_work(j, t, q, groups):
        def begin():
            w = [weight_ref[t, q, k] for k in range(8)]
            ends = (lane == 32 * q) | (lane == (32 * q - 1) % LANES)
            values = []
            for s in groups:
                middle, ahead, behind = parts(basis_ref, j, main_row(4 * s + q, t), w)
                middle = middle + jnp.where(ends, edge_ref[j % 2, t, s], 0.0)
                values.append((middle, pltpu.roll(ahead, LANES - 1, 1), pltpu.roll(behind, 1, 1)))
            return values

        def end(values):
            for s, (middle, ahead, behind) in zip(groups, values):
                basis_ref[j + 1, at8(main_row(4 * s + q, t)), :] = middle + ahead + behind

        return begin, end

    def span(j, n):
        low, high = (0, TILES) if j + 1 < ITERS else (1, TILES - 1)
        half = (high - low) // 2
        return [low + half * n + k for k in range(half)]

    staged([strip_work(0, t) for n in range(2) for t in span(0, n)])
    for j in range(ITERS):
        def body(n, _, j=j):
            work = [main_work(j, t, q, range(GROUPS)) for t in span(j, n) for q in range(4)]
            if j + 1 < ITERS:
                work += [strip_work(j + 1, t) for t in span(j + 1, n)]
            staged(work)
            return 0

        lax.fori_loop(0, 2, body, 0)

    def products(s, _):
        for q in range(4):
            m = 4 * s + q
            sums = [None] * len(PAIRS)
            for t in range(1, TILES - 1):
                u = [basis_ref[j, at8(main_row(m, t)), :] for j in range(BASIS)]
                d = diag_ref[q, 8 * (t - 1) : 8 * t]
                scaled = [d * u[j] for j in range(ITERS)]
                for n, (i, j) in enumerate(PAIRS):
                    term = scaled[i] * u[j]
                    sums[n] = term if sums[n] is None else sums[n] + term
            for n in range(len(PAIRS)):
                partial_ref[at8((n * MEMBERS + m) * 8), :] = sums[n]
        return 0

    lax.fori_loop(0, GROUPS, products, 0)
    result = zero
    for l in range(len(PAIRS) * MEMBERS // 8):
        rows = [partial_ref[pl.ds(64 * l + k, 8, stride=8), :] for k in range(8)]
        while len(rows) > 1:
            rows = [rows[k] + rows[k + 1] for k in range(0, len(rows), 2)]
        result = jnp.where(lane == l, jnp.sum(rows[0], axis=1, keepdims=True), result)
    for n in range(gram_ref.shape[0]):
        gram_ref[n] = result


def two_sum(a, b):
    s = a + b
    t = s - a
    return s, (a - (s - t)) + (b - t)


def quick(a, b):
    s = a + b
    return s, b - (s - a)


def halves(a):
    t = 4097.0 * a
    high = t - (t - a)
    return high, a - high


def add2(a, b):
    s, e = two_sum(a[0], b[0])
    return quick(s, e + (a[1] + b[1]))


def mul2(a, b):
    p = a[0] * b[0]
    ah, al = halves(a[0])
    bh, bl = halves(b[0])
    e = ((ah * bh - p) + ah * bl + al * bh) + al * bl
    return quick(p, e + (a[0] * b[1] + a[1] * b[0]))


def neg2(a):
    return -a[0], -a[1]


def div2(a, b):
    q = a[0] / b[0]
    zero = jnp.zeros_like(q)
    rest = add2(a, neg2(mul2((q, zero), b)))
    return quick(q, rest[0] / b[0])


def sum2(terms):
    terms = list(terms)
    while len(terms) > 1:
        terms = [add2(terms[k], terms[k + 1]) if k + 1 < len(terms) else terms[k] for k in range(0, len(terms), 2)]
    return terms[0]


def finish_kernel(total_ref, basis_ref, diag_ref, solved_ref, left_ref, coeff_ref, solution_ref, residual_ref, sems):
    count = total_ref.shape[0]
    high, low = sum2([(total_ref[n, 0], total_ref[n, 1]) for n in range(count)])
    gram = {}
    for n, (i, j) in enumerate(PAIRS):
        shift = (LANES - 4 * n) % LANES
        value = (high, low) if shift == 0 else (pltpu.roll(high, shift, 1), pltpu.roll(low, shift, 1))
        gram[i, j] = gram[j, i] = value

    def scaled(value, factor):
        if factor == 1.0:
            return value
        s, e = two_sum(0.5 * value[0], 0.125 * value[0])
        return quick(s, e + factor * value[1])

    def dot(a, b):
        return sum2([mul2(x, y) for x, y in zip(a, b)])

    one = (jnp.ones((8, LANES), F32), jnp.zeros((8, LANES), F32))
    precond, direction, answer = [one], [one], []
    rz = gram[0, 0]
    for k in range(ITERS):
        image = [scaled(c, 1.0 - SHIFT[j]) for j, c in enumerate(direction)]
        image = [image[0]] + [
            add2(image[j], neg2(direction[j - 1])) for j in range(1, k + 1)
        ] + [neg2(direction[k])]
        final = k + 1 == ITERS
        row = [dot([gram[i, j] for j in range(k + 2)], image) for i in range(k + 1 if final else k + 2)]
        step_size = div2(rz, dot(direction, row))
        moved = [mul2(step_size, c) for c in direction]
        answer = [add2(a, b) for a, b in zip(answer, moved)] + moved[len(answer):]
        if not final:
            cross = dot(precond, row)
            rz_new = mul2(step_size, add2(mul2(step_size, dot(image, row)), (-2.0 * cross[0], -2.0 * cross[1])))
            rz_new = add2(rz, rz_new)
        moved = [neg2(mul2(step_size, c)) for c in image]
        precond = [add2(a, b) for a, b in zip(precond, moved)] + moved[len(precond):]
        if not final:
            ratio = div2(rz_new, rz)
            moved = [mul2(ratio, c) for c in direction]
            direction = [add2(a, b) for a, b in zip(precond, moved)] + precond[len(moved):]
            rz = rz_new

    values = [c[0] for c in answer] + [c[0] for c in precond]
    for n, value in enumerate(values):
        for l in range(MEMBERS // 8):
            coeff_ref[n, 8 * l : 8 * l + 8] = jnp.broadcast_to(value[:, l : l + 1], (8, LANES))

    def combine(s, _):
        for q in range(4):
            m = 4 * s + q
            c = [jnp.broadcast_to(coeff_ref[n, pl.ds(m, 1), :], (8, LANES)) for n in range(2 * ITERS + 1)]
            for t in range(ROWS // 8):
                at = pl.multiple_of(16 + m * EXT + 8 * t, 8)
                u = [basis_ref[j, pl.ds(at, 8), :] for j in range(BASIS)]
                solved = c[0] * u[0]
                left = c[ITERS] * u[0]
                for j in range(1, BASIS):
                    if j < ITERS:
                        solved = solved + c[j] * u[j]
                    left = left + c[ITERS + j] * u[j]
                solution_ref[m, 8 * t : 8 * t + 8] = rolled(solved, -32 * q)
                residual_ref[m, 8 * t : 8 * t + 8] = rolled(diag_ref[q, 8 * t : 8 * t + 8] * left, -32 * q)
        for copy in copies(s):
            copy.start()
        return 0

    def copies(s):
        members = pl.ds(4 * s, 4)
        return [
            pltpu.make_async_copy(source.at[members], target.at[members], sems.at[n, s])
            for n, (source, target) in enumerate(((solution_ref, solved_ref), (residual_ref, left_ref)))
        ]

    lax.fori_loop(0, GROUPS, combine, 0, unroll=4)
    for s in range(GROUPS):
        for copy in copies(s):
            copy.wait()


def shape(*dims):
    return jax.ShapeDtypeStruct(dims, F32)


def call(kernel, inputs, out_shape, scratch=(), in_specs=None, out_specs=None):
    return pl.pallas_call(
        kernel,
        out_shape=out_shape,
        in_specs=in_specs or [VMEM] * len(inputs),
        out_specs=out_specs or [VMEM] * len(out_shape),
        scratch_shapes=list(scratch),
        interpret=INTERPRET,
        compiler_params=pltpu.CompilerParams(vmem_limit_bytes=28 * 1024 * 1024),
    )(*inputs)


def on_device(right_side, couplings, center, ocean_mask):
    ny, nx = lax.axis_size(GY), lax.axis_size(GX)
    top = (lax.axis_index(GY) == ny - 1).astype(jnp.int32).reshape(1)
    sent = shape(PACKED, LANES)
    right_side, couplings, center, ocean_mask = (
        pltpu.with_memory_space_constraint(a, pltpu.HBM) for a in (right_side, couplings, center, ocean_mask)
    )
    planes, last, first = call(
        edges_kernel, (right_side, couplings, center, ocean_mask), (shape(PLANES, ROWS, LANES), sent, sent),
        scratch=(
            pltpu.VMEM((2, MEMBERS, 8, LANES), F32),
            pltpu.VMEM((ROWS, LANES), F32),
            pltpu.VMEM((ROWS, LANES), jnp.int32),
            pltpu.SemaphoreType.DMA((5,)),
        ),
        in_specs=[HBM] * 4,
    )
    south = lax.ppermute(last, GY, [(k, k + 1) for k in range(ny - 1)])
    north = lax.ppermute(first, GY, [(k + 1, k) for k in range(ny - 1)])
    row = (ny - 1) * nx
    turned_last = last[::-1, ::-1]
    fold = lax.ppermute(turned_last, ALL, [(row + k, row + nx - 1 - k) for k in range(nx)])

    inner = shape(3, TILES - 2, 8, LANES)
    turned, inner_west, inner_east = call(
        pack_own_kernel, (right_side, planes), (shape(MEMBERS, ROWS, LANES), inner, inner),
        scratch=(pltpu.VMEM((MEMBERS, ROWS, LANES), F32), pltpu.SemaphoreType.DMA),
        in_specs=[HBM, VMEM],
    )
    packed = shape(2 * TILES + (TILES + 3) // 4, 8, LANES)
    turned_halo, planes_halo, own_west, own_east = call(
        pack_halo_kernel,
        (south, north, fold, inner_west, inner_east),
        (shape(MEMBERS, 2, 8, LANES), shape(PLANES, 2, 8, LANES), packed, packed),
        scratch=(
            pltpu.VMEM((2, MEMBERS, 8, LANES), F32),
            pltpu.VMEM((3, 2, 8, LANES), F32),
            pltpu.VMEM((3, 2, 8, LANES), F32),
        ),
    )
    from_west = lax.ppermute(own_east, GX, [(k, (k + 1) % nx) for k in range(nx)])
    from_east = lax.ppermute(own_west, GX, [((k + 1) % nx, k) for k in range(nx)])

    near, far = lax.axis_size(NEAR), lax.axis_size(FAR)
    basis, diag, gram = call(
        basis_kernel,
        (top, turned, turned_halo, planes, planes_halo, own_west, own_east, from_west, from_east),
        (shape(BASIS, 16 + MEMBERS * EXT, LANES), shape(4, ROWS, LANES), shape(near, 8, LANES)),
        scratch=(
            pltpu.VMEM((ITERS, 16 + GROUPS * EXT, LANES), F32),
            pltpu.VMEM((16 + PLANES * EXT, LANES), F32),
            pltpu.VMEM((16 + PLANES * EXT, LANES), F32),
            pltpu.VMEM((TILES, 4, 8, 8, LANES), F32),
            pltpu.VMEM((TILES, 8, 8, LANES), F32),
            pltpu.VMEM((TILES, 4, 8, LANES), F32),
            pltpu.VMEM((TILES, 8, LANES), F32),
            pltpu.VMEM((2, TILES, GROUPS, 8, LANES), F32),
            pltpu.VMEM((len(PAIRS) * MEMBERS * 8, LANES), F32),
        ),
        in_specs=[SMEM] + [VMEM] * 8,
    )
    parts = lax.all_to_all(gram, NEAR, 0, 0, tiled=True)
    zero = jnp.zeros((8, LANES), F32)
    mine = jnp.stack(sum2([(parts[k], zero) for k in range(near)]))
    total = lax.all_to_all(jnp.broadcast_to(mine[None], (far, *mine.shape)), FAR, 0, 0, tiled=True)
    return tuple(call(
        finish_kernel,
        (total, basis, diag),
        (shape(MEMBERS, ROWS, LANES), shape(MEMBERS, ROWS, LANES)),
        scratch=(
            pltpu.VMEM((2 * ITERS + 1, MEMBERS, LANES), F32),
            pltpu.VMEM((MEMBERS, ROWS, LANES), F32),
            pltpu.VMEM((MEMBERS, ROWS, LANES), F32),
            pltpu.SemaphoreType.DMA((2, GROUPS)),
        ),
        out_specs=[HBM, HBM],
    ))


def solution(mesh):
    split = Mesh(mesh.devices.reshape(8, 4, 4, 2), ("gy_0", "gy_1", "gx_0", "gx_1"))
    placed = (P(None, GY, GX), P(None, GY, GX), P(GY, GX), P(GY, GX))
    return jax.shard_map(
        on_device,
        mesh=split,
        in_specs=placed,
        out_specs=(P(None, GY, GX), P(None, GY, GX)),
        check_vma=False,
    )
```

```python
import jax
import jax.numpy as jnp
from jax import lax
from jax.experimental import pallas as pl
from jax.experimental.pallas import tpu as pltpu
from jax.sharding import Mesh
from jax.sharding import PartitionSpec as P


ITERS = 6
SHIFT = (0.375, 0.0, 0.375, 0.0, 0.375, 0.0)
GY = ("gy_0", "gy_1")
GX = ("gx_0", "gx_1")
ALL = GY + GX
NEAR = ("gy_0", "gx_1")
FAR = ("gy_1", "gx_0")
MEMBERS = 32
ROWS = 64
LANES = 128
HALO = 8
TILES = (ROWS + 2 * HALO) // 8
EXT = ROWS + 2 * HALO
GROUPS = MEMBERS // 4
PLANES = 4
BASIS = ITERS + 1
PAIRS = [(i, j) for i in range(ITERS) for j in range(i, BASIS)]
INTERPRET = False
F32 = jnp.float32
VMEM = pl.BlockSpec(memory_space=pltpu.VMEM)
SMEM = pl.BlockSpec(memory_space=pltpu.SMEM)
HBM = pl.BlockSpec(memory_space=pltpu.HBM)


def lanes_of():
    return lax.broadcasted_iota(jnp.int32, (8, LANES), 1)


def rolled(value, shift):
    shift %= LANES
    return value if shift == 0 else pltpu.roll(value, shift, 1)


SENT = 6
PACKED = MEMBERS * SENT + PLANES * 8


def edges_kernel(
    right_ref, couplings_ref, center_ref, mask_ref, planes_ref, last_ref, first_ref, rows_ref, center_row_ref, mask_row_ref, sems
):
    copies = [
        pltpu.make_async_copy(couplings_ref, planes_ref.at[pl.ds(0, 3)], sems.at[0]),
        pltpu.make_async_copy(center_ref, center_row_ref, sems.at[1]),
        pltpu.make_async_copy(mask_ref, mask_row_ref, sems.at[2]),
        pltpu.make_async_copy(right_ref.at[:, pl.ds(ROWS - 8, 8), :], rows_ref.at[0], sems.at[3]),
        pltpu.make_async_copy(right_ref.at[:, pl.ds(0, 8), :], rows_ref.at[1], sems.at[4]),
    ]
    for copy in copies:
        copy.start()
    for copy in copies:
        copy.wait()
    planes_ref[3] = jnp.where(mask_row_ref[...] != 0, center_row_ref[...], 0.0)
    for p in range(PLANES):
        base = MEMBERS * SENT + 8 * p
        last_ref[base : base + 8] = planes_ref[p, ROWS - 8 : ROWS]
        first_ref[base : base + 8] = planes_ref[p, 0:8]
    for m in range(MEMBERS):
        last_ref[SENT * m : SENT * m + SENT] = rows_ref[0, m, 8 - SENT : 8]
        first_ref[SENT * m : SENT * m + SENT] = rows_ref[1, m, 0:SENT]


def pack(load, store, west_ref, east_ref, tile):
    window = lanes_of() // 8
    for h in range(3):
        members = range(16 * h, 16 * h + 16) if h < 2 else range(MEMBERS, MEMBERS + PLANES)
        first = last = None
        for m in members:
            value = rolled(load(m), 32 * (m % 4))
            if m < MEMBERS:
                store(m, value)
            extra = 8 * (m // 4 % 4) if h < 2 else 0
            low, high = rolled(value, extra), rolled(value, extra + 8)
            if first is None:
                first, last = low, high
            else:
                here = window == 4 * (m % 4) + extra // 8
                first = jnp.where(here, low, first)
                last = jnp.where(here, high, last)
        west_ref[h, tile] = first
        east_ref[h, tile] = last


def pack_own_kernel(right_hbm_ref, planes_ref, turned_ref, west_ref, east_ref, right_ref, sem):
    def fetch(t):
        rows = pl.ds(8 * t if isinstance(t, int) else pl.multiple_of(8 * t, 8), 8)
        return pltpu.make_async_copy(right_hbm_ref.at[:, rows, :], right_ref.at[:, rows, :], sem.at[t])

    for t in range(ROWS // 8):
        fetch(t).start()

    def own(t, _):
        at = pl.multiple_of(8 * t, 8)
        fetch(t).wait()

        def load(m):
            return right_ref[m, pl.ds(at, 8), :] if m < MEMBERS else planes_ref[m - MEMBERS, pl.ds(at, 8), :]

        def store(m, value):
            turned_ref[m, pl.ds(at, 8), :] = value

        pack(load, store, west_ref, east_ref, t)
        return 0

    lax.fori_loop(0, ROWS // 8, own, 0)


def pack_halo_kernel(
    south_ref, north_ref, fold_ref, own_west_ref, own_east_ref, turned_ref, planes_ref, west_ref, east_ref, rows_ref,
    ends_west_ref, ends_east_ref,
):
    for h in range(2):
        west_ref[TILES * h + 1 : TILES * (h + 1) - 1] = own_west_ref[h]
        east_ref[TILES * h + 1 : TILES * (h + 1) - 1] = own_east_ref[h]
    zero = jnp.zeros((8, LANES), F32)
    for m in range(MEMBERS):
        rows_ref[0, m] = zero
        rows_ref[1, m] = zero
        rows_ref[0, m, 8 - SENT : 8] = south_ref[SENT * m : SENT * m + SENT]
        back = PACKED - SENT * (m + 1)
        rows_ref[1, m, 0:SENT] = north_ref[SENT * m : SENT * m + SENT] + fold_ref[back : back + SENT]
    for p in range(PLANES):
        base = MEMBERS * SENT + 8 * p
        back = PACKED - base - 8
        planes_ref[p, 0] = south_ref[base : base + 8]
        planes_ref[p, 1] = north_ref[base : base + 8] + fold_ref[back : back + 8]
    for k, tile in ((0, 0), (1, TILES - 1)):
        def load(m, k=k):
            return rows_ref[k, m] if m < MEMBERS else planes_ref[m - MEMBERS, k]

        def store(m, value, k=k):
            turned_ref[m, k] = value

        pack(load, store, ends_west_ref, ends_east_ref, k)
        for h in range(2):
            west_ref[TILES * h + tile] = ends_west_ref[h, k]
            east_ref[TILES * h + tile] = ends_east_ref[h, k]
    part = lanes_of() % 32 // 8
    for out_ref, own_ref, ends_ref in ((west_ref, own_west_ref, ends_west_ref), (east_ref, own_east_ref, ends_east_ref)):
        for n in range((TILES + 3) // 4):
            value = None
            for tile in range(4 * n, min(4 * n + 4, TILES)):
                one = ends_ref[2, 0] if tile == 0 else ends_ref[2, 1] if tile == TILES - 1 else own_ref[2, tile - 1]
                one = rolled(one, 8 * (tile % 4))
                value = one if value is None else jnp.where(part == tile % 4, one, value)
            out_ref[2 * TILES + n] = value


def basis_kernel(
    top_ref, right_ref, right_halo_ref, planes_ref, planes_halo_ref,
    own_west_ref, own_east_ref, from_west_ref, from_east_ref,
    basis_ref, diag_ref, gram_ref,
    strip_ref, plane_ref, plane_strip_ref, weight_ref, weight_strip_ref, inverse_ref, inverse_strip_ref,
    edge_ref, partial_ref,
):
    lane = lanes_of()
    spot = (lane + 7) % 32

    def main_row(member, tile):
        return 8 + member * EXT + 8 * tile

    def at8(row):
        return pl.ds(pl.multiple_of(row, 8), 8)

    zero = jnp.zeros((8, LANES), F32)
    for j in range(ITERS):
        basis_ref[j, 0:8] = zero
        basis_ref[j, 8 + MEMBERS * EXT : 16 + MEMBERS * EXT] = zero
        strip_ref[j, 0:8] = zero
        strip_ref[j, 8 + GROUPS * EXT : 16 + GROUPS * EXT] = zero

    for p in range(PLANES):
        base = 8 + p * EXT
        plane_ref[base : base + 8] = planes_halo_ref[p, 0]
        plane_ref[base + 8 : base + 8 + ROWS] = planes_ref[p]
        plane_ref[base + 8 + ROWS : base + EXT] = planes_halo_ref[p, 1]
    plane_ref[0:8] = zero
    plane_ref[8 + PLANES * EXT : 16 + PLANES * EXT] = zero
    plane_strip_ref[0:8] = zero
    plane_strip_ref[8 + PLANES * EXT : 16 + PLANES * EXT] = zero

    def joined(n, at):
        out = rolled(from_west_ref[n], -7 - at)
        out = jnp.where(spot < 8, out, rolled(own_west_ref[n], 1 - at))
        out = jnp.where(spot < 16, out, rolled(own_east_ref[n], 9 - at))
        return jnp.where(spot < 24, out, rolled(from_east_ref[n], 17 - at))

    for t in range(TILES):
        value = joined(2 * TILES + t // 4, 8 * (t % 4))
        for p in range(PLANES):
            one = jnp.where((lane + 7) // 32 % 4 == p, value, 0.0)
            one = one + pltpu.roll(one, 32, 1)
            one = one + pltpu.roll(one, 64, 1)
            plane_strip_ref[8 + p * EXT + 8 * t : 16 + p * EXT + 8 * t] = one

    def weights(t, ghost):
        dr = 1 if ghost else -1
        side = LANES - 1 if ghost else 1

        def row(ref, p, shift):
            return ref[pl.ds(8 + p * EXT + 8 * t + shift, 8), :]

        def beside(main, strip):
            if ghost:
                return jnp.where(lane == LANES - 1, pltpu.roll(strip, 110, 1), pltpu.roll(main, side, 1))
            return jnp.where(lane == 0, strip, pltpu.roll(main, side, 1))

        def finish(cn0, cnr, ce0, cec, cc0, ccr, ccc, ccrc, center, main):
            total = center + cn0 + cnr + ce0 + cec + cc0 + ccr + ccc + ccrc
            inv = jnp.where(center > 0.0, 1.0 / total, 0.0)
            if ghost:
                w = dict(s=cn0, n=cnr, w=ce0, e=cec, sw=cc0, nw=ccr, se=ccc, ne=ccrc)
            else:
                w = dict(n=cn0, s=cnr, e=ce0, w=cec, ne=cc0, se=ccr, nw=ccc, sw=ccrc)

            def ahead(value):
                value = pltpu.roll(value * inv, 1, 1)
                return jnp.where(lane == 0, 0.0, value) if main else value

            def behind(value):
                value = pltpu.roll(value * inv, LANES - 1, 1)
                return jnp.where(lane == LANES - 1, 0.0, value) if main else value

            return total, inv, (
                w["s"] * inv, w["n"] * inv,
                ahead(w["se"]), ahead(w["e"]), ahead(w["ne"]),
                behind(w["sw"]), behind(w["w"]), behind(w["nw"]),
            )

        strips = [row(plane_strip_ref, p, 0) for p in range(PLANES)]
        strips_r = [row(plane_strip_ref, p, dr) for p in (0, 2)]
        _, inv, ws = finish(
            strips[0], strips_r[0], strips[1], pltpu.roll(strips[1], side, 1),
            strips[2], strips_r[1], pltpu.roll(strips[2], side, 1), pltpu.roll(strips_r[1], side, 1),
            strips[3], False,
        )
        inverse_strip_ref[t] = inv
        for k in range(8):
            weight_strip_ref[t, k] = ws[k]
        mains = [row(plane_ref, p, 0) for p in range(PLANES)]
        mains_r = [row(plane_ref, p, dr) for p in (0, 2)]
        total, inv, ws = finish(
            mains[0], mains_r[0], mains[1], beside(mains[1], strips[1]),
            mains[2], mains_r[1], beside(mains[2], strips[2]), beside(mains_r[1], strips_r[1]),
            mains[3], True,
        )
        for q in range(4):
            inverse_ref[t, q] = rolled(inv, 32 * q)
            for k in range(8):
                weight_ref[t, q, k] = rolled(ws[k], 32 * q)
        return total

    weights(0, False)

    def inner_weights(t, _):
        total = weights(t, False)
        for q in range(4):
            diag_ref[q, at8(8 * (t - 1)), :] = rolled(total, 32 * q)
        return 0

    lax.fori_loop(1, TILES - 1, inner_weights, 0, unroll=True)

    @pl.when(top_ref[0] == 0)
    def _():
        weights(TILES - 1, False)

    @pl.when(top_ref[0] != 0)
    def _():
        weights(TILES - 1, True)

    def first(t, load):
        for q in range(4):
            inv = inverse_ref[t, q]
            for s in range(GROUPS):
                m = 4 * s + q
                basis_ref[0, at8(main_row(m, t)), :] = load(m) * inv
        inv = inverse_strip_ref[t]
        for s in range(GROUPS):
            strip_ref[0, at8(8 + s * EXT + 8 * t), :] = joined(TILES * (s // 4) + t, 8 * (s % 4)) * inv

    first(0, lambda m: right_halo_ref[m, 0])

    def inner_first(t, _):
        first(t, lambda m: right_ref[m, at8(8 * (t - 1)), :])
        return 0

    lax.fori_loop(1, TILES - 1, inner_first, 0, unroll=True)
    first(TILES - 1, lambda m: right_halo_ref[m, 1])

    def parts(ref, j, base, w):
        a = ref[j, pl.ds(base - 1, 8), :]
        b = ref[j, at8(base), :]
        c = ref[j, pl.ds(base + 1, 8), :]
        middle = w[0] * a + w[1] * c
        if SHIFT[j]:
            middle = middle - SHIFT[j] * b
        return middle, (w[2] * a + w[4] * c) + w[3] * b, (w[5] * a + w[7] * c) + w[6] * b

    def staged(work):
        begun = [(end, begin()) for begin, end in work]
        for end, values in begun:
            end(values)

    def strip_work(j, t):
        def begin():
            w = [weight_strip_ref[t, k] for k in range(8)]
            values = []
            for s in range(GROUPS):
                middle, ahead, behind = parts(strip_ref, j, 8 + s * EXT + 8 * t, w)
                edge = jnp.where(lane % 32 == 31, pltpu.roll(ahead, LANES - 18, 1), behind)
                moved = (pltpu.roll(ahead, LANES - 1, 1), pltpu.roll(behind, 1, 1)) if j + 1 < ITERS else ()
                values.append((middle, edge, moved))
            return values

        def end(values):
            for s, (middle, edge, moved) in enumerate(values):
                edge_ref[j % 2, t, s] = edge
                if moved:
                    strip_ref[j + 1, at8(8 + s * EXT + 8 * t), :] = middle + moved[0] + moved[1]

        return begin, end

    def main_work(j, t, q, groups):
        def begin():
            w = [weight_ref[t, q, k] for k in range(8)]
            ends = (lane == 32 * q) | (lane == (32 * q - 1) % LANES)
            values = []
            for s in groups:
                middle, ahead, behind = parts(basis_ref, j, main_row(4 * s + q, t), w)
                middle = middle + jnp.where(ends, edge_ref[j % 2, t, s], 0.0)
                values.append((middle, pltpu.roll(ahead, LANES - 1, 1), pltpu.roll(behind, 1, 1)))
            return values

        def end(values):
            for s, (middle, ahead, behind) in zip(groups, values):
                basis_ref[j + 1, at8(main_row(4 * s + q, t)), :] = middle + ahead + behind

        return begin, end

    def span(j, n):
        low, high = (0, TILES) if j + 1 < ITERS else (1, TILES - 1)
        half = (high - low) // 2
        return [low + half * n + k for k in range(half)]

    staged([strip_work(0, t) for n in range(2) for t in span(0, n)])
    for j in range(ITERS):
        def body(n, _, j=j):
            work = [main_work(j, t, q, range(GROUPS)) for t in span(j, n) for q in range(4)]
            if j + 1 < ITERS:
                work += [strip_work(j + 1, t) for t in span(j + 1, n)]
            staged(work)
            return 0

        lax.fori_loop(0, 2, body, 0)

    def products(s, _):
        for q in range(4):
            m = 4 * s + q
            sums = [None] * len(PAIRS)
            for t in range(1, TILES - 1):
                u = [basis_ref[j, at8(main_row(m, t)), :] for j in range(BASIS)]
                d = diag_ref[q, 8 * (t - 1) : 8 * t]
                scaled = [d * u[j] for j in range(ITERS)]
                for n, (i, j) in enumerate(PAIRS):
                    term = scaled[i] * u[j]
                    sums[n] = term if sums[n] is None else sums[n] + term
            for n in range(len(PAIRS)):
                partial_ref[at8((n * MEMBERS + m) * 8), :] = sums[n]
        return 0

    lax.fori_loop(0, GROUPS, products, 0)
    result = zero
    for l in range(len(PAIRS) * MEMBERS // 8):
        rows = [partial_ref[pl.ds(64 * l + k, 8, stride=8), :] for k in range(8)]
        while len(rows) > 1:
            rows = [rows[k] + rows[k + 1] for k in range(0, len(rows), 2)]
        result = jnp.where(lane == l, jnp.sum(rows[0], axis=1, keepdims=True), result)
    for n in range(gram_ref.shape[0]):
        gram_ref[n] = result


def two_sum(a, b):
    s = a + b
    t = s - a
    return s, (a - (s - t)) + (b - t)


def quick(a, b):
    s = a + b
    return s, b - (s - a)


def halves(a):
    t = 4097.0 * a
    high = t - (t - a)
    return high, a - high


def add2(a, b):
    s, e = two_sum(a[0], b[0])
    return quick(s, e + (a[1] + b[1]))


def mul2(a, b):
    p = a[0] * b[0]
    ah, al = halves(a[0])
    bh, bl = halves(b[0])
    e = ((ah * bh - p) + ah * bl + al * bh) + al * bl
    return quick(p, e + (a[0] * b[1] + a[1] * b[0]))


def neg2(a):
    return -a[0], -a[1]


def div2(a, b):
    q = a[0] / b[0]
    zero = jnp.zeros_like(q)
    rest = add2(a, neg2(mul2((q, zero), b)))
    return quick(q, rest[0] / b[0])


def sum2(terms):
    terms = list(terms)
    while len(terms) > 1:
        terms = [add2(terms[k], terms[k + 1]) if k + 1 < len(terms) else terms[k] for k in range(0, len(terms), 2)]
    return terms[0]


def finish_kernel(total_ref, basis_ref, diag_ref, solved_ref, left_ref, coeff_ref, solution_ref, residual_ref, sems):
    count = total_ref.shape[0]
    high, low = sum2([(total_ref[n, 0], total_ref[n, 1]) for n in range(count)])
    gram = {}
    for n, (i, j) in enumerate(PAIRS):
        shift = (LANES - 4 * n) % LANES
        value = (high, low) if shift == 0 else (pltpu.roll(high, shift, 1), pltpu.roll(low, shift, 1))
        gram[i, j] = gram[j, i] = value

    def scaled(value, factor):
        if factor == 1.0:
            return value
        s, e = two_sum(0.5 * value[0], 0.125 * value[0])
        return quick(s, e + factor * value[1])

    def dot(a, b):
        return sum2([mul2(x, y) for x, y in zip(a, b)])

    one = (jnp.ones((8, LANES), F32), jnp.zeros((8, LANES), F32))
    precond, direction, answer = [one], [one], []
    rz = gram[0, 0]
    for k in range(ITERS):
        image = [scaled(c, 1.0 - SHIFT[j]) for j, c in enumerate(direction)]
        image = [image[0]] + [
            add2(image[j], neg2(direction[j - 1])) for j in range(1, k + 1)
        ] + [neg2(direction[k])]
        final = k + 1 == ITERS
        row = [dot([gram[i, j] for j in range(k + 2)], image) for i in range(k + 1 if final else k + 2)]
        step_size = div2(rz, dot(direction, row))
        moved = [mul2(step_size, c) for c in direction]
        answer = [add2(a, b) for a, b in zip(answer, moved)] + moved[len(answer):]
        if not final:
            cross = dot(precond, row)
            rz_new = mul2(step_size, add2(mul2(step_size, dot(image, row)), (-2.0 * cross[0], -2.0 * cross[1])))
            rz_new = add2(rz, rz_new)
        moved = [neg2(mul2(step_size, c)) for c in image]
        precond = [add2(a, b) for a, b in zip(precond, moved)] + moved[len(precond):]
        if not final:
            ratio = div2(rz_new, rz)
            moved = [mul2(ratio, c) for c in direction]
            direction = [add2(a, b) for a, b in zip(precond, moved)] + precond[len(moved):]
            rz = rz_new

    values = [c[0] for c in answer] + [c[0] for c in precond]
    for n, value in enumerate(values):
        for l in range(MEMBERS // 8):
            coeff_ref[n, 8 * l : 8 * l + 8] = jnp.broadcast_to(value[:, l : l + 1], (8, LANES))

    def combine(s, _):
        for q in range(4):
            m = 4 * s + q
            c = [jnp.broadcast_to(coeff_ref[n, pl.ds(m, 1), :], (8, LANES)) for n in range(2 * ITERS + 1)]
            for t in range(ROWS // 8):
                at = pl.multiple_of(16 + m * EXT + 8 * t, 8)
                u = [basis_ref[j, pl.ds(at, 8), :] for j in range(BASIS)]
                solved = c[0] * u[0]
                left = c[ITERS] * u[0]
                for j in range(1, BASIS):
                    if j < ITERS:
                        solved = solved + c[j] * u[j]
                    left = left + c[ITERS + j] * u[j]
                solution_ref[m, 8 * t : 8 * t + 8] = rolled(solved, -32 * q)
                residual_ref[m, 8 * t : 8 * t + 8] = rolled(diag_ref[q, 8 * t : 8 * t + 8] * left, -32 * q)
        for copy in copies(s):
            copy.start()
        return 0

    def copies(s):
        members = pl.ds(4 * s, 4)
        return [
            pltpu.make_async_copy(source.at[members], target.at[members], sems.at[n, s])
            for n, (source, target) in enumerate(((solution_ref, solved_ref), (residual_ref, left_ref)))
        ]

    lax.fori_loop(0, GROUPS, combine, 0, unroll=4)
    for s in range(GROUPS):
        for copy in copies(s):
            copy.wait()


def shape(*dims):
    return jax.ShapeDtypeStruct(dims, F32)


def call(kernel, inputs, out_shape, scratch=(), in_specs=None, out_specs=None):
    return pl.pallas_call(
        kernel,
        out_shape=out_shape,
        in_specs=in_specs or [VMEM] * len(inputs),
        out_specs=out_specs or [VMEM] * len(out_shape),
        scratch_shapes=list(scratch),
        interpret=INTERPRET,
        compiler_params=pltpu.CompilerParams(vmem_limit_bytes=28 * 1024 * 1024),
    )(*inputs)


def on_device(right_side, couplings, center, ocean_mask):
    ny, nx = lax.axis_size(GY), lax.axis_size(GX)
    top = (lax.axis_index(GY) == ny - 1).astype(jnp.int32).reshape(1)
    sent = shape(PACKED, LANES)
    right_side, couplings, center, ocean_mask = (
        pltpu.with_memory_space_constraint(a, pltpu.HBM) for a in (right_side, couplings, center, ocean_mask)
    )
    planes, last, first = call(
        edges_kernel, (right_side, couplings, center, ocean_mask), (shape(PLANES, ROWS, LANES), sent, sent),
        scratch=(
            pltpu.VMEM((2, MEMBERS, 8, LANES), F32),
            pltpu.VMEM((ROWS, LANES), F32),
            pltpu.VMEM((ROWS, LANES), jnp.int32),
            pltpu.SemaphoreType.DMA((5,)),
        ),
        in_specs=[HBM] * 4,
    )
    south = lax.ppermute(last, GY, [(k, k + 1) for k in range(ny - 1)])
    north = lax.ppermute(first, GY, [(k + 1, k) for k in range(ny - 1)])
    row = (ny - 1) * nx
    turned_last = last[::-1, ::-1]
    fold = lax.ppermute(turned_last, ALL, [(row + k, row + nx - 1 - k) for k in range(nx)])

    inner = shape(3, TILES - 2, 8, LANES)
    turned, inner_west, inner_east = call(
        pack_own_kernel, (right_side, planes), (shape(MEMBERS, ROWS, LANES), inner, inner),
        scratch=(pltpu.VMEM((MEMBERS, ROWS, LANES), F32), pltpu.SemaphoreType.DMA((ROWS // 8,))),
        in_specs=[HBM, VMEM],
    )
    packed = shape(2 * TILES + (TILES + 3) // 4, 8, LANES)
    turned_halo, planes_halo, own_west, own_east = call(
        pack_halo_kernel,
        (south, north, fold, inner_west, inner_east),
        (shape(MEMBERS, 2, 8, LANES), shape(PLANES, 2, 8, LANES), packed, packed),
        scratch=(
            pltpu.VMEM((2, MEMBERS, 8, LANES), F32),
            pltpu.VMEM((3, 2, 8, LANES), F32),
            pltpu.VMEM((3, 2, 8, LANES), F32),
        ),
    )
    from_west = lax.ppermute(own_east, GX, [(k, (k + 1) % nx) for k in range(nx)])
    from_east = lax.ppermute(own_west, GX, [((k + 1) % nx, k) for k in range(nx)])

    near, far = lax.axis_size(NEAR), lax.axis_size(FAR)
    basis, diag, gram = call(
        basis_kernel,
        (top, turned, turned_halo, planes, planes_halo, own_west, own_east, from_west, from_east),
        (shape(BASIS, 16 + MEMBERS * EXT, LANES), shape(4, ROWS, LANES), shape(near, 8, LANES)),
        scratch=(
            pltpu.VMEM((ITERS, 16 + GROUPS * EXT, LANES), F32),
            pltpu.VMEM((16 + PLANES * EXT, LANES), F32),
            pltpu.VMEM((16 + PLANES * EXT, LANES), F32),
            pltpu.VMEM((TILES, 4, 8, 8, LANES), F32),
            pltpu.VMEM((TILES, 8, 8, LANES), F32),
            pltpu.VMEM((TILES, 4, 8, LANES), F32),
            pltpu.VMEM((TILES, 8, LANES), F32),
            pltpu.VMEM((2, TILES, GROUPS, 8, LANES), F32),
            pltpu.VMEM((len(PAIRS) * MEMBERS * 8, LANES), F32),
        ),
        in_specs=[SMEM] + [VMEM] * 8,
    )
    parts = lax.all_to_all(gram, NEAR, 0, 0, tiled=True)
    zero = jnp.zeros((8, LANES), F32)
    mine = jnp.stack(sum2([(parts[k], zero) for k in range(near)]))
    total = lax.all_to_all(jnp.broadcast_to(mine[None], (far, *mine.shape)), FAR, 0, 0, tiled=True)
    return tuple(call(
        finish_kernel,
        (total, basis, diag),
        (shape(MEMBERS, ROWS, LANES), shape(MEMBERS, ROWS, LANES)),
        scratch=(
            pltpu.VMEM((2 * ITERS + 1, MEMBERS, LANES), F32),
            pltpu.VMEM((MEMBERS, ROWS, LANES), F32),
            pltpu.VMEM((MEMBERS, ROWS, LANES), F32),
            pltpu.SemaphoreType.DMA((2, GROUPS)),
        ),
        out_specs=[HBM, HBM],
    ))


def solution(mesh):
    split = Mesh(mesh.devices.reshape(8, 4, 4, 2), ("gy_0", "gy_1", "gx_0", "gx_1"))
    placed = (P(None, GY, GX), P(None, GY, GX), P(GY, GX), P(GY, GX))
    return jax.shard_map(
        on_device,
        mesh=split,
        in_specs=placed,
        out_specs=(P(None, GY, GX), P(None, GY, GX)),
        check_vma=False,
    )
```
